128 devices in a mesh: row: 8 (over x_hi, z), col: 16 (over x_lo, y, core).
Axes of the slice: x: 4 (x_hi: 2, x_lo: 2; x = x_hi * 2 + x_lo), y: 4, z: 4, core: 2. Of those that a mesh axis runs over, the one named last changes fastest.
Arguments:
- tokens: bfloat16 [1024, 12288], P('row', 'col'), may hold values from -6 to 6
- prev_tokens: bfloat16 [1024, 12288], P('row', 'col'), may hold values from -6 to 6
- hidden_grad: bfloat16 [1024, 49152], P('col', 'row'), may hold values from -6 to 6
- active_blocks: int32 [1], replicated, may hold values from 6 to 16
- weight: bfloat16 [12288, 49152], P('col', 'row'), may hold values from -0.0546875 to 0.0546875
Outputs:
- activation: bfloat16 [1024, 49152], P('col', 'row')
- weight_grad: bfloat16 [12288, 49152], P('col', 'row')
The draws below stay inside these ranges and needn't reach their ends.
Inputs may be any that keep to these rules, and one draw needn't show every extreme that they name: The sampled blocks are the first active_blocks[0] blocks of 3072 hidden units.
All inputs are finite; a program needn't handle non-finite values.
Results may differ from the reference program's by a relative error of at most 0.001.
Values may be sent and summed in bfloat16 or wider, within the bound.
A program may use at most 640 MiB of HBM per device.

```python
import jax
import jax.numpy as jnp
from jax import lax

D = 12288
FF = 49152
BLOCK = 3072
TOKENS = 1024
DSLAB = 768
N_COL = 16


def shard_levels(stream_key, extent, shards, least, largest):
    def one(dim, blocks):
        steps = jax.random.uniform(jax.random.fold_in(jax.random.fold_in(stream_key, 6), dim), (blocks,), jnp.float32, least / len(shards), largest / len(shards))
        return jnp.repeat(jnp.exp(steps), extent[dim] // blocks).reshape((-1,) + (1,) * (len(extent) - dim - 1))

    loudness = one(*shards[0])
    for cut in shards[1:]:
        loudness = loudness * one(*cut)
    return loudness


def gaussian(own_key, extent, spread, bound, pieces=(), held_as=jnp.bfloat16):
    array = jax.random.normal(own_key, extent, jnp.float32) * spread
    if len(pieces) > 0:
        array = shard_levels(own_key, extent, pieces, -0.22, 0.18) * array
    return jnp.clip(array, min=-bound, max=bound).astype(held_as)


def setup_inputs(seed: int = 0) -> dict:
    seeds = jax.random.split(jax.random.key(seed), 6)
    return {
        "tokens": gaussian(seeds[0], (TOKENS, D), 1.0, 6.0, ((0, 8), (1, 16))),
        "prev_tokens": gaussian(seeds[1], (TOKENS, D), 1.0, 6.0, ((0, 8), (1, 16))),
        "hidden_grad": gaussian(seeds[2], (TOKENS, FF), 1.0, 6.0, ((0, 16), (1, 8))),
        "active_blocks": jax.random.randint(seeds[3], (1,), 6, 17).astype(jnp.int32),
        "weight": gaussian(seeds[4], (D, FF), D ** -0.5, 0.0546875, ((0, 16), (1, 8))),
    }


def reference(tokens, prev_tokens, hidden_grad, active_blocks, weight):
    unit_limit = active_blocks[0] * BLOCK
    unit_mask = (jnp.arange(FF, dtype=jnp.int32) < unit_limit).astype(jnp.float32)

    def add_slab(running, index):
        columns = lax.dynamic_slice_in_dim(tokens, (index * DSLAB).astype(jnp.int32), DSLAB, 1)
        weight_rows = lax.dynamic_slice_in_dim(weight, (index * DSLAB).astype(jnp.int32), DSLAB, 0)
        partial_value = jnp.dot(columns, weight_rows, preferred_element_type=jnp.float32)
        return running + partial_value, None

    hidden, unused = lax.scan(add_slab, jnp.zeros((TOKENS, FF), jnp.float32), jnp.arange(N_COL, dtype=jnp.int32))
    activation = (jax.nn.gelu(hidden, approximate=False) * unit_mask).astype(jnp.bfloat16)

    def grad_block(index):
        offset = (index * BLOCK).astype(jnp.int32)
        grad_cols = lax.dynamic_slice_in_dim(hidden_grad, offset, BLOCK, 1)
        mask_cols = lax.dynamic_slice_in_dim(unit_mask, offset, BLOCK, 0)
        block_grad = lax.dot_general(prev_tokens, grad_cols, (((0,), (0,)), ((), ())), preferred_element_type=jnp.float32)
        return (block_grad * mask_cols).astype(jnp.bfloat16)

    blocks = lax.map(grad_block, jnp.arange(FF // BLOCK, dtype=jnp.int32))
    weight_grad = jnp.transpose(blocks, (1, 0, 2)).reshape(D, FF)
    return activation, weight_grad
```

```python
import jax
import jax.numpy as jnp
from jax import lax
from jax.experimental import pallas as pl
from jax.experimental.pallas import tpu as pltpu
from jax.sharding import PartitionSpec as P

BLOCK = 3072
MESH = pl.DeviceIdType.MESH
TB = 128
A_COLS = 1024
A_PIECES = ((0, 512), (512, 512))
B_PIECES = ((1024, 1024), (2048, 1024))
GA = 3584
GSTEP = 512
N_COPIES = 96


def kernel(tok, prev, hg, w, hid, g, xs, pv, pvt, ws, gs, part, gst,
           ax_s, ax_r, ay_s, ay_r, by_s, by_r, bx_s, bx_r,
           axs_s, axs_r, ays_s, ays_r, bys_s, bys_r, bxs_s, bxs_r,
           ssem, rsem, lsem, gsem):
    row, col = lax.axis_index("row"), lax.axis_index("col")
    z, c = lax.rem(row, 4), lax.rem(col, 2)
    half = lax.div(col, 2)
    y, xl = lax.rem(half, 4), lax.div(half, 4)
    zb, yb = row - z, xl * 8 + c
    yp, ym, y2 = lax.rem(y + 1, 4), lax.rem(y + 3, 4), lax.rem(y + 2, 4)
    zp, zm, z2 = lax.rem(z + 1, 4), lax.rem(z + 3, 4), lax.rem(z + 2, 4)
    xo = 1 - xl
    rowx = lax.rem(row + 4, 8)
    zbx = rowx - z
    d_cp = (row, col + 1 - 2 * c)
    d_xp = (row, lax.rem(col + 8, 16))
    d_yp, d_ym = (row, yb + yp * 2), (row, yb + ym * 2)
    d_hx = (rowx, col)
    d_zp, d_zm = (zb + zp, col), (zb + zm, col)

    barrier = pltpu.get_barrier_semaphore()
    peers = (d_cp, d_xp, d_yp, d_ym, d_hx, d_zp, d_zm)
    for d in peers:
        pl.semaphore_signal(barrier, inc=1, device_id=d, device_id_type=MESH)
    pl.semaphore_wait(barrier, len(peers))

    sent = []

    def send(src, dst, dev):
        k = len(sent)
        copy = pltpu.make_async_remote_copy(
            src_ref=src, dst_ref=dst, send_sem=ssem.at[k], recv_sem=rsem.at[k],
            device_id=dev, device_id_type=MESH)
        copy.start()
        sent.append(copy)
        return copy

    def local(k, src, dst):
        copy = pltpu.make_async_copy(src, dst, lsem.at[k])
        copy.start()
        return copy

    def got(*copies):
        for copy in copies:
            copy.wait_recv()

    slab = pl.ds(pl.multiple_of(c * 768, 128), 768)
    mine = pl.ds(pl.multiple_of(c * 3072, 128), 3072)
    other = pl.ds(pl.multiple_of((1 - c) * 3072, 128), 3072)
    ca, cb = pl.ds(0, GA), pl.ds(GA, 6144 - GA)
    hb = (6144 - GA) // 2
    cb0, cb1 = pl.ds(GA, hb), pl.ds(GA + hb, hb)

    def xrow(r):
        return xs.at[r, :, slab]

    def grow(xx, yy, cols):
        return gs.at[xx * 4 + yy, c, :, cols]

    t_x = send(tok, xrow(row), d_hx)
    t_op = send(tok, xrow(row), d_zp)
    t_om = send(tok, xrow(row), d_zm)
    h_x = send(hg.at[:, ca], grow(xl, y, ca), d_xp)
    h_op = send(hg.at[:, ca], grow(xl, y, ca), d_yp)
    h_om = send(hg.at[:, ca], grow(xl, y, ca), d_ym)
    w_c = send(w.at[:, other], ws.at[slab, :], d_cp)
    t_c = [send(tok, xrow(row), d_cp)]
    b_op = send(hg.at[:, cb], grow(xl, y, cb), d_yp)
    b_om = send(hg.at[:, cb], grow(xl, y, cb), d_ym)
    b_x = [send(hg.at[:, cb], grow(xl, y, cb), d_xp)]
    l_t = local(0, tok, xrow(row))
    l_w = local(1, w.at[:, mine], ws.at[slab, :])
    l_h = local(2, hg, gs.at[xl * 4 + y, c])
    l_p = local(3, prev, pv.at[row])

    got(t_x)
    t_pp = send(xrow(rowx), xrow(rowx), d_zp)
    t_pm = send(xrow(rowx), xrow(rowx), d_zm)
    t_c.append(send(xrow(rowx), xrow(rowx), d_cp))
    p_x = send(prev, pv.at[row], d_hx)
    got(h_x)
    h_pp = send(grow(xo, y, ca), grow(xo, y, ca), d_yp)
    h_pm = send(grow(xo, y, ca), grow(xo, y, ca), d_ym)
    got(t_op, t_om)
    t_f0 = send(xrow(zb + zm), xrow(zb + zm), d_zp)
    t_c.append(send(xrow(zb + zm), xrow(zb + zm), d_cp))
    t_c.append(send(xrow(zb + zp), xrow(zb + zp), d_cp))
    got(h_op, h_om)
    h_f0 = send(grow(xl, ym, ca), grow(xl, ym, ca), d_yp)
    got(t_pp, t_pm)
    t_f1 = send(xrow(zbx + zp), xrow(zbx + zp), d_zm)
    t_c.append(send(xrow(zbx + zm), xrow(zbx + zm), d_cp))
    t_c.append(send(xrow(zbx + zp), xrow(zbx + zp), d_cp))
    p_op = send(prev, pv.at[row], d_zp)
    p_om = send(prev, pv.at[row], d_zm)
    got(b_op, b_om)
    b_f0 = send(grow(xl, ym, cb0), grow(xl, ym, cb0), d_yp)
    b_f1 = send(grow(xl, yp, cb1), grow(xl, yp, cb1), d_ym)
    b_x.append(send(grow(xl, ym, cb), grow(xl, ym, cb), d_xp))
    b_x.append(send(grow(xl, yp, cb), grow(xl, yp, cb), d_xp))
    got(t_f0, t_f1)
    t_c.append(send(xrow(zb + z2), xrow(zb + z2), d_cp))
    t_c.append(send(xrow(zbx + z2), xrow(zbx + z2), d_cp))
    l_t.wait()
    l_w.wait()
    got(w_c, *t_c)

    def product(lo, hi):
        def tile(i, carry):
            cols = pl.ds(pl.multiple_of(i * 256, 256), 256)
            part[:, cols] = jnp.dot(
                xs[...].reshape(1024, 1536), ws[:, cols], preferred_element_type=jnp.float32)
            return carry

        lax.fori_loop(lo // 256, hi // 256, tile, 0)

    def prow(xx, yy):
        return pl.ds(pl.multiple_of((xx * 4 + yy) * TB, TB), TB)

    def quant(rows, c0, n, q, s):
        def peak(k, m):
            v = part[rows, pl.ds(pl.multiple_of(c0 + k * 128, 128), 128)]
            return jnp.maximum(m, jnp.max(jnp.abs(v.reshape(16, 8, 128)), axis=0))

        m = lax.fori_loop(0, n // 128, peak, jnp.full((8, 128), 1e-30, jnp.float32))
        s[...] = m * (1.0 / 32766.0)
        inv = 32766.0 / m

        def code(k, carry):
            v = part[rows, pl.ds(pl.multiple_of(c0 + k * 128, 128), 128)]
            v = (v.reshape(16, 8, 128) * inv[None]).reshape(TB, 128)
            q[:, pl.ds(pl.multiple_of(k * 128, 128), 128)] = (
                jnp.round(v).astype(jnp.int32).astype(jnp.int16))
            return carry

        lax.fori_loop(0, n // 128, code, 0)

    def add(rows, c0, n, q, s):
        def step(k, carry):
            cols = pl.ds(pl.multiple_of(c0 + k * 128, 128), 128)
            v = q[:, pl.ds(pl.multiple_of(k * 128, 128), 128)].astype(jnp.int32).astype(jnp.float32)
            v = (v.reshape(16, 8, 128) * s[...][None]).reshape(TB, 128)
            part[rows, cols] = part[rows, cols] + v
            return carry

        lax.fori_loop(0, n // 128, step, 0)

    def send2(qs, ss, qr, sr, dev):
        return send(ss, sr, dev), send(qs, qr, dev)

    def a_first(i):
        c0, n = A_PIECES[i]
        for yy in range(4):
            quant(prow(xo, yy), c0, n, ax_s.at[i, yy], axs_s.at[i, yy])
        return send2(ax_s.at[i], axs_s.at[i], ax_r.at[i], axs_r.at[i], d_xp)

    def a_second(i, first):
        c0, n = A_PIECES[i]
        yd, yo, d_d, d_o = (yp, ym, d_yp, d_ym) if i % 2 == 0 else (ym, yp, d_ym, d_yp)
        got(*first)
        for yy in range(4):
            add(prow(xl, yy), c0, n, ax_r.at[i, yy], axs_r.at[i, yy])
        far = by_y(ay_s, ay_r, ays_s, ays_r, i, 0, prow(xl, y2), c0, n, d_d)
        near = by_y(ay_s, ay_r, ays_s, ays_r, i, 1, prow(xl, yo), c0, n, d_o)
        return far, near

    def by_y(qs, qr, ss, sr, i, k, rows, c0, n, dev):
        quant(rows, c0, n, qs.at[i, k], ss.at[i, k])
        return send2(qs.at[i, k], ss.at[i, k], qr.at[i, k], sr.at[i, k], dev)

    def a_third(i, far):
        c0, n = A_PIECES[i]
        yd, d_d = (yp, d_yp) if i % 2 == 0 else (ym, d_ym)
        got(*far)
        add(prow(xl, yd), c0, n, ay_r.at[i, 0], ays_r.at[i, 0])
        return by_y(ay_s, ay_r, ays_s, ays_r, i, 2, prow(xl, yd), c0, n, d_d)

    def a_last(i, near, passed):
        c0, n = A_PIECES[i]
        got(*near, *passed)
        add(prow(xl, y), c0, n, ay_r.at[i, 1], ays_r.at[i, 1])
        add(prow(xl, y), c0, n, ay_r.at[i, 2], ays_r.at[i, 2])

    def b_y(i, k, rows, dev):
        c0, n = B_PIECES[i]
        return by_y(by_s, by_r, bys_s, bys_r, i, k, rows, c0, n, dev)

    def b_first(i):
        return (b_y(i, 0, prow(0, y2), d_yp), b_y(i, 1, prow(1, y2), d_ym),
                b_y(i, 2, prow(1, yp), d_yp), b_y(i, 3, prow(0, ym), d_ym))

    def b_second(i, first):
        c0, n = B_PIECES[i]
        got(*first[0])
        add(prow(0, yp), c0, n, by_r.at[i, 0], bys_r.at[i, 0])
        up = b_y(i, 4, prow(0, yp), d_yp)
        got(*first[1])
        add(prow(1, ym), c0, n, by_r.at[i, 1], bys_r.at[i, 1])
        down = b_y(i, 5, prow(1, ym), d_ym)
        return up, down

    def b_third(i, first, second):
        c0, n = B_PIECES[i]
        got(*first[2], *first[3])
        add(prow(1, y), c0, n, by_r.at[i, 2], bys_r.at[i, 2])
        add(prow(0, y), c0, n, by_r.at[i, 3], bys_r.at[i, 3])
        got(*second[0], *second[1])
        add(prow(0, y), c0, n, by_r.at[i, 4], bys_r.at[i, 4])
        add(prow(1, y), c0, n, by_r.at[i, 5], bys_r.at[i, 5])
        quant(prow(xo, y), c0, n, bx_s.at[i], bxs_s.at[i])
        return send2(bx_s.at[i], bxs_s.at[i], bx_r.at[i], bxs_r.at[i], d_xp)

    def b_last(i, third):
        c0, n = B_PIECES[i]
        got(*third)
        add(prow(xl, y), c0, n, bx_r.at[i], bxs_r.at[i])

    def grad(lo, hi):
        def tile(i, carry):
            cols = pl.ds(pl.multiple_of(i * GSTEP, GSTEP), GSTEP)
            slot = lax.rem(i, 2)

            @pl.when(i >= 2)
            def _():
                pltpu.make_async_copy(gst.at[slot], g.at[:, cols], gsem.at[slot]).wait()

            gst[slot] = jnp.dot(
                pvt[...], gs[:, :, :, cols].reshape(1024, GSTEP),
                preferred_element_type=jnp.float32).astype(jnp.bfloat16)
            pltpu.make_async_copy(gst.at[slot], g.at[:, cols], gsem.at[slot]).start()
            return carry

        lax.fori_loop(lo, hi, tile, 0)

    product(0, A_COLS)
    a1 = [a_first(0), a_first(1)]
    got(h_pp, h_pm)
    h_f1 = send(grow(xo, yp, ca), grow(xo, yp, ca), d_ym)
    got(p_x)
    p_pp = send(pv.at[rowx], pv.at[rowx], d_zp)
    p_pm = send(pv.at[rowx], pv.at[rowx], d_zm)
    product(B_PIECES[0][0], B_PIECES[0][0] + B_PIECES[0][1])
    b1 = [b_first(0)]
    got(b_f0, b_f1)
    b_x.append(send(grow(xl, y2, cb), grow(xl, y2, cb), d_xp))
    got(p_op, p_om)
    p_f0 = send(pv.at[zb + zm], pv.at[zb + zm], d_zp)
    product(B_PIECES[1][0], B_PIECES[1][0] + B_PIECES[1][1])
    b1.append(b_first(1))
    got(p_pp, p_pm)
    p_f1 = send(pv.at[zbx + zp], pv.at[zbx + zp], d_zm)
    got(h_f0, h_f1)
    l_h.wait()
    c_a = send(gs.at[:, c, :, ca], gs.at[:, c, :, ca], d_cp)
    got(*b_x)
    c_b = send(gs.at[:, c, :, cb], gs.at[:, c, :, cb], d_cp)
    l_p.wait()
    got(p_f0, p_f1)
    pvt[...] = pv[...].reshape(1024, 768).T
    b2 = [b_second(0, b1[0])]
    n_grad = 6144 // GSTEP
    got(c_a, c_b)
    a2 = [a_second(0, a1[0])]
    b2.append(b_second(1, b1[1]))
    grad(0, n_grad // 3)
    a2.append(a_second(1, a1[1]))
    a3 = [a_third(0, a2[0][0])]
    b3 = [b_third(0, b1[0], b2[0])]
    grad(n_grad // 3, 2 * n_grad // 3)
    a3.append(a_third(1, a2[1][0]))
    b3.append(b_third(1, b1[1], b2[1]))
    grad(2 * n_grad // 3, n_grad)
    for i in range(2):
        b_last(i, b3[i])
    for i in range(2):
        a_last(i, a2[i][1], a3[i])

    own = pl.ds(pl.multiple_of((xl * 4 + y) * TB + c * 64, 64), 64)
    theirs = pl.ds(pl.multiple_of((xl * 4 + y) * TB + (1 - c) * 64, 64), 64)
    last = send(part.at[theirs, :], hid.at[:, mine], d_cp)
    l_o = local(4, part.at[own, :], hid.at[:, mine])
    for slot in range(2):
        pltpu.make_async_copy(gst.at[slot], g.at[:, pl.ds(0, GSTEP)], gsem.at[slot]).wait()
    l_o.wait()
    got(last)
    for copy in sent:
        copy.wait_send()


def exchange(tokens, prev_tokens, hidden_grad, weight):
    bf, f32, i16 = jnp.bfloat16, jnp.float32, jnp.int16
    any_space = pl.BlockSpec(memory_space=pl.ANY)
    na, nb = A_PIECES[0][1], B_PIECES[0][1]

    def pair(shape, dtype):
        return [pltpu.VMEM(shape, dtype)] * 2

    return pl.pallas_call(
        kernel,
        out_shape=(
            jax.ShapeDtypeStruct((64, 6144), f32),
            jax.ShapeDtypeStruct((768, 6144), bf),
        ),
        in_specs=[any_space] * 4,
        out_specs=(any_space, any_space),
        scratch_shapes=[
            pltpu.VMEM((8, 128, 1536), bf),
            pltpu.VMEM((8, 128, 768), bf),
            pltpu.VMEM((768, 1024), bf),
            pltpu.VMEM((1536, 3072), bf),
            pltpu.VMEM((8, 2, 64, 6144), bf),
            pltpu.VMEM((1024, 3072), f32),
            pltpu.VMEM((2, 768, GSTEP), bf),
            *pair((2, 4, TB, na), i16),
            *pair((2, 3, TB, na), i16),
            *pair((2, 6, TB, nb), i16),
            *pair((2, TB, nb), i16),
            *pair((2, 4, 8, 128), f32),
            *pair((2, 3, 8, 128), f32),
            *pair((2, 6, 8, 128), f32),
            *pair((2, 8, 128), f32),
            pltpu.SemaphoreType.DMA((N_COPIES,)),
            pltpu.SemaphoreType.DMA((N_COPIES,)),
            pltpu.SemaphoreType.DMA((5,)),
            pltpu.SemaphoreType.DMA((2,)),
        ],
        compiler_params=pltpu.CompilerParams(
            collective_id=0, has_side_effects=True, vmem_limit_bytes=67043328),
    )(tokens, prev_tokens, hidden_grad, weight)


def shards(tokens, prev_tokens, hidden_grad, active_blocks, weight):
    local_units = weight.shape[1]
    first_unit = lax.axis_index("row") * local_units
    unit_ids = first_unit + lax.iota(jnp.int32, local_units)
    active = unit_ids < active_blocks[0] * BLOCK
    hidden, grad = exchange(tokens, prev_tokens, hidden_grad, weight)
    activation = jnp.where(active, jax.nn.gelu(hidden, approximate=False), 0.0).astype(jnp.bfloat16)
    weight_grad = jnp.where(active, grad, jnp.zeros((), jnp.bfloat16))
    return (activation, weight_grad)


def solution(mesh):
    return jax.shard_map(
        shards,
        mesh=mesh,
        in_specs=(P("row", "col"), P("row", "col"), P("col", "row"), P(), P("col", "row")),
        out_specs=(P("col", "row"), P("col", "row")),
        check_vma=False,
    )
```

```python
import jax
import jax.numpy as jnp
from jax import lax
from jax.experimental import pallas as pl
from jax.experimental.pallas import tpu as pltpu
from jax.sharding import PartitionSpec as P

BLOCK = 3072
MESH = pl.DeviceIdType.MESH
TB = 128
A_COLS = 1024
A_PIECES = ((0, 512), (512, 512))
B_PIECES = ((1024, 512), (1536, 512), (2048, 512), (2560, 512))
GA = 3584
GSTEP = 512
N_COPIES = 136
VMEM_LIMIT = 54 * 1000 * 1000


def kernel(active, tok, prev, hg, w, act, g, xs, pv, pvt, gs, part, actv,
           ax_s, ax_r, ay_s, ay_r, by_s, by_r, bx_s, bx_r,
           axs_s, axs_r, ays_s, ays_r, bys_s, bys_r, bxs_s, bxs_r,
           ssem, rsem, lsem):
    row, col = lax.axis_index("row"), lax.axis_index("col")
    z, c = lax.rem(row, 4), lax.rem(col, 2)
    half = lax.div(col, 2)
    y, xl = lax.rem(half, 4), lax.div(half, 4)
    zb, yb = row - z, xl * 8 + c
    yp, ym, y2 = lax.rem(y + 1, 4), lax.rem(y + 3, 4), lax.rem(y + 2, 4)
    zp, zm, z2 = lax.rem(z + 1, 4), lax.rem(z + 3, 4), lax.rem(z + 2, 4)
    xo = 1 - xl
    rowx = lax.rem(row + 4, 8)
    zbx = rowx - z
    d_cp = (row, col + 1 - 2 * c)
    d_xp = (row, lax.rem(col + 8, 16))
    d_yp, d_ym = (row, yb + yp * 2), (row, yb + ym * 2)
    d_hx = (rowx, col)
    d_zp, d_zm = (zb + zp, col), (zb + zm, col)

    barrier = pltpu.get_barrier_semaphore()
    peers = (d_cp, d_xp, d_yp, d_ym, d_hx, d_zp, d_zm)
    for d in peers:
        pl.semaphore_signal(barrier, inc=1, device_id=d, device_id_type=MESH)
    pl.semaphore_wait(barrier, len(peers))

    sent = []

    def send(src, dst, dev):
        k = len(sent)
        copy = pltpu.make_async_remote_copy(
            src_ref=src, dst_ref=dst, send_sem=ssem.at[k], recv_sem=rsem.at[k],
            device_id=dev, device_id_type=MESH)
        copy.start()
        sent.append(copy)
        return copy

    def local(k, src, dst):
        copy = pltpu.make_async_copy(src, dst, lsem.at[k])
        copy.start()
        return copy

    def got(*copies):
        for copy in copies:
            copy.wait_recv()

    slab = pl.ds(pl.multiple_of(c * 768, 128), 768)
    mine = pl.ds(pl.multiple_of(c * 3072, 128), 3072)
    other = pl.ds(pl.multiple_of((1 - c) * 3072, 128), 3072)
    ca, cb = pl.ds(0, GA), pl.ds(GA, 6144 - GA)
    hb = (6144 - GA) // 2
    cb0, cb1 = pl.ds(GA, hb), pl.ds(GA + hb, hb)

    def xrow(r):
        return xs.at[r, :, slab]

    def grow(xx, yy, cols):
        return gs.at[xx * 4 + yy, c, :, cols]

    t_x = send(tok, xrow(row), d_hx)
    t_op = send(tok, xrow(row), d_zp)
    t_om = send(tok, xrow(row), d_zm)
    h_x = send(hg.at[:, ca], grow(xl, y, ca), d_xp)
    h_op = send(hg.at[:, ca], grow(xl, y, ca), d_yp)
    h_om = send(hg.at[:, ca], grow(xl, y, ca), d_ym)
    w_c = send(w.at[:, other], g.at[:, mine], d_cp)
    t_c = [send(tok, xrow(row), d_cp)]
    b_op = send(hg.at[:, cb], grow(xl, y, cb), d_yp)
    b_om = send(hg.at[:, cb], grow(xl, y, cb), d_ym)
    b_x = [send(hg.at[:, cb], grow(xl, y, cb), d_xp)]
    l_t = local(0, tok, xrow(row))
    l_w = local(1, w.at[:, mine], g.at[:, mine])
    l_h = local(2, hg, gs.at[xl * 4 + y, c])
    l_p = local(3, prev, pv.at[row])

    got(t_x)
    t_pp = send(xrow(rowx), xrow(rowx), d_zp)
    t_pm = send(xrow(rowx), xrow(rowx), d_zm)
    t_c.append(send(xrow(rowx), xrow(rowx), d_cp))
    p_x = send(prev, pv.at[row], d_hx)
    got(t_op, t_om)
    t_f0 = send(xrow(zb + zm), xrow(zb + zm), d_zp)
    t_c.append(send(xrow(zb + zm), xrow(zb + zm), d_cp))
    t_c.append(send(xrow(zb + zp), xrow(zb + zp), d_cp))
    got(t_pp, t_pm)
    t_f1 = send(xrow(zbx + zp), xrow(zbx + zp), d_zm)
    t_c.append(send(xrow(zbx + zm), xrow(zbx + zm), d_cp))
    t_c.append(send(xrow(zbx + zp), xrow(zbx + zp), d_cp))
    p_op = send(prev, pv.at[row], d_zp)
    p_om = send(prev, pv.at[row], d_zm)
    got(h_x)
    h_pp = send(grow(xo, y, ca), grow(xo, y, ca), d_yp)
    h_pm = send(grow(xo, y, ca), grow(xo, y, ca), d_ym)
    got(h_op, h_om)
    h_f0 = send(grow(xl, ym, ca), grow(xl, ym, ca), d_yp)
    got(b_op, b_om)
    b_f1 = send(grow(xl, yp, cb1), grow(xl, yp, cb1), d_ym)
    b_f0 = send(grow(xl, ym, cb0), grow(xl, ym, cb0), d_yp)
    b_x.append(send(grow(xl, ym, cb), grow(xl, ym, cb), d_xp))
    b_x.append(send(grow(xl, yp, cb), grow(xl, yp, cb), d_xp))
    got(t_f0, t_f1)
    t_c.append(send(xrow(zb + z2), xrow(zb + z2), d_cp))
    t_c.append(send(xrow(zbx + z2), xrow(zbx + z2), d_cp))
    l_t.wait()
    l_w.wait()
    got(w_c, *t_c)

    def product(lo, hi):
        def tile(i, carry):
            cols = pl.ds(pl.multiple_of(i * 256, 256), 256)
            cols2 = pl.ds(pl.multiple_of(i * 256 + 3072, 256), 256)
            part[:, cols] = jnp.dot(
                xs[...].reshape(1024, 1536),
                jnp.concatenate([g[:, cols], g[:, cols2]], axis=0),
                preferred_element_type=jnp.float32)
            return carry

        lax.fori_loop(lo // 256, hi // 256, tile, 0)

    def prow(xx, yy):
        return pl.ds(pl.multiple_of((xx * 4 + yy) * TB, TB), TB)

    def quant(rows, c0, n, q, s):
        def peak(k, m):
            v = part[rows, pl.ds(pl.multiple_of(c0 + k * 128, 128), 128)]
            return jnp.maximum(m, jnp.max(jnp.abs(v.reshape(16, 8, 128)), axis=0))

        m = lax.fori_loop(0, n // 128, peak, jnp.full((8, 128), 1e-30, jnp.float32))
        s[...] = m * (1.0 / 32766.0)
        inv = 32766.0 / m

        def code(k, carry):
            v = part[rows, pl.ds(pl.multiple_of(c0 + k * 128, 128), 128)]
            v = (v.reshape(16, 8, 128) * inv[None]).reshape(TB, 128)
            q[:, pl.ds(pl.multiple_of(k * 128, 128), 128)] = (
                jnp.round(v).astype(jnp.int32).astype(jnp.int16))
            return carry

        lax.fori_loop(0, n // 128, code, 0)

    def add(rows, c0, n, q, s):
        def step(k, carry):
            cols = pl.ds(pl.multiple_of(c0 + k * 128, 128), 128)
            v = q[:, pl.ds(pl.multiple_of(k * 128, 128), 128)].astype(jnp.int32).astype(jnp.float32)
            v = (v.reshape(16, 8, 128) * s[...][None]).reshape(TB, 128)
            part[rows, cols] = part[rows, cols] + v
            return carry

        lax.fori_loop(0, n // 128, step, 0)

    def send2(qs, ss, qr, sr, dev):
        return send(ss, sr, dev), send(qs, qr, dev)

    def a_first(i):
        c0, n = A_PIECES[i]
        for yy in range(4):
            quant(prow(xo, yy), c0, n, ax_s.at[i, yy], axs_s.at[i, yy])
        return send2(ax_s.at[i], axs_s.at[i], ax_r.at[i], axs_r.at[i], d_xp)

    def a_second(i, first):
        c0, n = A_PIECES[i]
        yd, yo, d_d, d_o = (yp, ym, d_yp, d_ym) if i % 2 == 0 else (ym, yp, d_ym, d_yp)
        got(*first)
        for yy in range(4):
            add(prow(xl, yy), c0, n, ax_r.at[i, yy], axs_r.at[i, yy])
        far = by_y(ay_s, ay_r, ays_s, ays_r, i, 0, prow(xl, y2), c0, n, d_d)
        near = by_y(ay_s, ay_r, ays_s, ays_r, i, 1, prow(xl, yo), c0, n, d_o)
        return far, near

    def by_y(qs, qr, ss, sr, i, k, rows, c0, n, dev):
        quant(rows, c0, n, qs.at[i, k], ss.at[i, k])
        return send2(qs.at[i, k], ss.at[i, k], qr.at[i, k], sr.at[i, k], dev)

    def a_third(i, far):
        c0, n = A_PIECES[i]
        yd, d_d = (yp, d_yp) if i % 2 == 0 else (ym, d_ym)
        got(*far)
        add(prow(xl, yd), c0, n, ay_r.at[i, 0], ays_r.at[i, 0])
        return by_y(ay_s, ay_r, ays_s, ays_r, i, 2, prow(xl, yd), c0, n, d_d)

    def a_last(i, near, passed):
        c0, n = A_PIECES[i]
        got(*near, *passed)
        add(prow(xl, y), c0, n, ay_r.at[i, 1], ays_r.at[i, 1])
        add(prow(xl, y), c0, n, ay_r.at[i, 2], ays_r.at[i, 2])
        finish(c0, n)

    def b_y(i, k, rows, dev):
        c0, n = B_PIECES[i]
        return by_y(by_s, by_r, bys_s, bys_r, i, k, rows, c0, n, dev)

    def b_first(i):
        return b_y(i, 0, prow(0, y2), d_yp), b_y(i, 1, prow(1, y2), d_ym)

    def b_near(i):
        return b_y(i, 2, prow(1, yp), d_yp), b_y(i, 3, prow(0, ym), d_ym)

    def b_second(i, first):
        c0, n = B_PIECES[i]
        got(*first[0])
        add(prow(0, yp), c0, n, by_r.at[i, 0], bys_r.at[i, 0])
        up = b_y(i, 4, prow(0, yp), d_yp)
        got(*first[1])
        add(prow(1, ym), c0, n, by_r.at[i, 1], bys_r.at[i, 1])
        down = b_y(i, 5, prow(1, ym), d_ym)
        return up, down

    def b_third(i, near, second):
        c0, n = B_PIECES[i]
        got(*near[0], *near[1])
        add(prow(1, y), c0, n, by_r.at[i, 2], bys_r.at[i, 2])
        add(prow(0, y), c0, n, by_r.at[i, 3], bys_r.at[i, 3])
        got(*second[0], *second[1])
        add(prow(0, y), c0, n, by_r.at[i, 4], bys_r.at[i, 4])
        add(prow(1, y), c0, n, by_r.at[i, 5], bys_r.at[i, 5])
        quant(prow(xo, y), c0, n, bx_s.at[i], bxs_s.at[i])
        return send2(bx_s.at[i], bxs_s.at[i], bx_r.at[i], bxs_r.at[i], d_xp)

    def b_last(i, third):
        c0, n = B_PIECES[i]
        got(*third)
        add(prow(xl, y), c0, n, bx_r.at[i], bxs_r.at[i])
        finish(c0, n)

    unit_limit = active[0] * BLOCK - row * 6144

    def unit_mask(first, rows, n):
        return first + lax.broadcasted_iota(jnp.int32, (rows, n), 1) < unit_limit

    def grad(lo, hi):
        def tile(i, carry):
            cols = pl.ds(pl.multiple_of(i * GSTEP, GSTEP), GSTEP)
            v = jnp.dot(pvt[...], gs[:, :, :, cols].reshape(1024, GSTEP),
                        preferred_element_type=jnp.float32)
            g[:, cols] = jnp.where(unit_mask(i * GSTEP, 768, GSTEP), v, 0.0).astype(jnp.bfloat16)
            return carry

        lax.fori_loop(lo, hi, tile, 0)

    own_rows = pl.ds(pl.multiple_of(c * 64, 64), 64)
    their_rows = pl.ds(pl.multiple_of((1 - c) * 64, 64), 64)
    finals = []

    def finish(c0, n):
        def step(k, carry):
            at = pl.multiple_of(c0 + k * 128, 128)
            v = part[prow(xl, y), pl.ds(at, 128)]
            v = v * (lax.erf(v * 0.7071067811865476) + 1.0) * 0.5
            v = jnp.where(unit_mask(c * 3072 + at, TB, 128), v, 0.0)
            actv[:, pl.ds(at, 128)] = v.astype(jnp.bfloat16)
            return carry

        lax.fori_loop(0, n // 128, step, 0)
        cols = pl.ds(pl.multiple_of(c * 3072 + c0, 128), n)
        finals.append(send(actv.at[their_rows, pl.ds(c0, n)], act.at[:, cols], d_cp))
        act[:, cols] = actv[own_rows, pl.ds(c0, n)]

    product(0, A_COLS)
    a1 = [a_first(i) for i in range(len(A_PIECES))]
    product(B_PIECES[0][0], B_PIECES[2][0])
    b1 = [b_first(0), b_first(1)]
    got(h_pp, h_pm)
    h_f1 = send(grow(xo, yp, ca), grow(xo, yp, ca), d_ym)
    got(p_x)
    p_pp = send(pv.at[rowx], pv.at[rowx], d_zp)
    p_pm = send(pv.at[rowx], pv.at[rowx], d_zm)
    got(b_f1)
    b_x.append(send(grow(xl, y2, cb1), grow(xl, y2, cb1), d_xp))
    product(B_PIECES[2][0], 3072)
    b1 += [b_first(2), b_first(3)]
    got(p_op, p_om)
    p_f0 = send(pv.at[zb + zm], pv.at[zb + zm], d_zp)
    b1n = [b_near(i) for i in range(4)]
    got(p_pp, p_pm)
    p_f1 = send(pv.at[zbx + zp], pv.at[zbx + zp], d_zm)
    got(h_f0)
    got(b_f0)
    b_x.append(send(grow(xl, y2, cb0), grow(xl, y2, cb0), d_xp))
    l_h.wait()
    near_rows, far_rows = pl.ds(xl * 4, 4), pl.ds(xo * 4, 4)
    c_b0 = send(gs.at[near_rows, c, :, cb], gs.at[near_rows, c, :, cb], d_cp)
    got(h_f1)
    c_a = send(gs.at[:, c, :, ca], gs.at[:, c, :, ca], d_cp)
    b2 = [b_second(0, b1[0])]
    l_p.wait()
    got(p_f0, p_f1)
    pvt[...] = pv[...].reshape(1024, 768).T
    b2.append(b_second(1, b1[1]))
    a2 = [a_second(0, a1[0])]
    got(c_a)
    grad(0, 1)
    b2.append(b_second(2, b1[2]))
    grad(1, 2)
    b2.append(b_second(3, b1[3]))
    grad(2, 4)
    a2.append(a_second(1, a1[1]))
    grad(4, 7)
    b3 = [b_third(0, b1n[0], b2[0])]
    got(*b_x)
    c_b1 = send(gs.at[far_rows, c, :, cb], gs.at[far_rows, c, :, cb], d_cp)
    b3.append(b_third(1, b1n[1], b2[1]))
    a3 = [a_third(0, a2[0][0])]
    got(c_b0, c_b1)
    grad(7, 9)
    b3.append(b_third(2, b1n[2], b2[2]))
    grad(9, 10)
    b3.append(b_third(3, b1n[3], b2[3]))
    a3.append(a_third(1, a2[1][0]))
    grad(10, 12)
    b_last(0, b3[0])
    b_last(1, b3[1])
    a_last(0, a2[0][1], a3[0])
    b_last(2, b3[2])
    b_last(3, b3[3])
    a_last(1, a2[1][1], a3[1])
    got(*finals)
    for copy in sent:
        copy.wait_send()


def exchange(active_blocks, tokens, prev_tokens, hidden_grad, weight):
    bf, f32, i16 = jnp.bfloat16, jnp.float32, jnp.int16
    any_space = pl.BlockSpec(memory_space=pl.ANY)
    vmem = pl.BlockSpec(memory_space=pltpu.VMEM)
    na, nb = A_PIECES[0][1], B_PIECES[0][1]
    pa, pb = len(A_PIECES), len(B_PIECES)

    def pair(shape, dtype):
        return [pltpu.VMEM(shape, dtype)] * 2

    return pl.pallas_call(
        kernel,
        out_shape=(pltpu.VMEM((64, 6144), bf), pltpu.VMEM((768, 6144), bf)),
        in_specs=[pl.BlockSpec(memory_space=pltpu.SMEM)] + [any_space] * 4,
        out_specs=(vmem, vmem),
        scratch_shapes=[
            pltpu.VMEM((8, 128, 1536), bf),
            pltpu.VMEM((8, 128, 768), bf),
            pltpu.VMEM((768, 1024), bf),
            pltpu.VMEM((8, 2, 64, 6144), bf),
            pltpu.VMEM((1024, 3072), f32),
            pltpu.VMEM((TB, 3072), bf),
            *pair((pa, 4, TB, na), i16),
            *pair((pa, 3, TB, na), i16),
            *pair((pb, 6, TB, nb), i16),
            *pair((pb, TB, nb), i16),
            *pair((pa, 4, 8, 128), f32),
            *pair((pa, 3, 8, 128), f32),
            *pair((pb, 6, 8, 128), f32),
            *pair((pb, 8, 128), f32),
            pltpu.SemaphoreType.DMA((N_COPIES,)),
            pltpu.SemaphoreType.DMA((N_COPIES,)),
            pltpu.SemaphoreType.DMA((4,)),
        ],
        compiler_params=pltpu.CompilerParams(
            collective_id=0, has_side_effects=True, vmem_limit_bytes=VMEM_LIMIT),
    )(active_blocks, *(pltpu.with_memory_space_constraint(a, pltpu.HBM)
                       for a in (tokens, prev_tokens, hidden_grad, weight)))


def store_kernel(act, g, act_out, g_out, sems):
    copies = [pltpu.make_async_copy(act, act_out, sems.at[4])]
    for k in range(4):
        rows = pl.ds(k * 192, 192)
        copies.append(pltpu.make_async_copy(g.at[rows], g_out.at[rows], sems.at[k]))
    for copy in copies:
        copy.start()
    for copy in copies:
        copy.wait()


def store(act, g):
    return pl.pallas_call(
        store_kernel,
        out_shape=(jax.ShapeDtypeStruct(act.shape, act.dtype), jax.ShapeDtypeStruct(g.shape, g.dtype)),
        in_specs=[pl.BlockSpec(memory_space=pltpu.VMEM)] * 2,
        out_specs=[pl.BlockSpec(memory_space=pl.ANY)] * 2,
        scratch_shapes=[pltpu.SemaphoreType.DMA((5,))],
        compiler_params=pltpu.CompilerParams(vmem_limit_bytes=12 * 1024 * 1024),
    )(act, g)


def shards(tokens, prev_tokens, hidden_grad, active_blocks, weight):
    act, grad = exchange(active_blocks, tokens, prev_tokens, hidden_grad, weight)
    return tuple(store(act, grad))


def solution(mesh):
    return jax.shard_map(
        shards,
        mesh=mesh,
        in_specs=(P("row", "col"), P("row", "col"), P("col", "row"), P(), P("col", "row")),
        out_specs=(P("col", "row"), P("col", "row")),
        check_vma=False,
    )
```

```python
import jax
import jax.numpy as jnp
from jax import lax
from jax.experimental import pallas as pl
from jax.experimental.pallas import tpu as pltpu
from jax.sharding import PartitionSpec as P

BLOCK = 3072
MESH = pl.DeviceIdType.MESH
TB = 128
A_COLS = 1024
A_PIECES = ((0, 512), (512, 512))
B_PIECES = ((1024, 512), (1536, 512), (2048, 512), (2560, 512))
GA = 3584
GSTEP = 512
N_COPIES = 95
N_SENDS = 65
VMEM_LIMIT = 54 * 1000 * 1000


def kernel(active, tok, prev, hg, w, act, g, xs, pv, pvt, gs, part, oth,
           ax_s, ax_r, ay_s, ay_r, by_s, by_r, bx_s, af_r, bf_r,
           ssem, rsem, lsem):
    row, col = lax.axis_index("row"), lax.axis_index("col")
    z, c = lax.rem(row, 4), lax.rem(col, 2)
    half = lax.div(col, 2)
    y, xl = lax.rem(half, 4), lax.div(half, 4)
    zb, yb = row - z, xl * 8 + c
    yp, ym, y2 = lax.rem(y + 1, 4), lax.rem(y + 3, 4), lax.rem(y + 2, 4)
    zp, zm, z2 = lax.rem(z + 1, 4), lax.rem(z + 3, 4), lax.rem(z + 2, 4)
    xo = 1 - xl
    rowx = lax.rem(row + 4, 8)
    zbx = rowx - z
    d_cp = (row, col + 1 - 2 * c)
    d_xp = (row, lax.rem(col + 8, 16))
    d_yp, d_ym = (row, yb + yp * 2), (row, yb + ym * 2)
    d_hx = (rowx, col)
    d_zp, d_zm = (zb + zp, col), (zb + zm, col)

    barrier = pltpu.get_barrier_semaphore()
    peers = (d_cp, d_xp, d_yp, d_ym, d_hx, d_zp, d_zm)
    for d in peers:
        pl.semaphore_signal(barrier, inc=1, device_id=d, device_id_type=MESH)
    pl.semaphore_wait(barrier, len(peers))

    sent, slots, free = [], [], list(range(N_SENDS))

    def send(src, dst, dev):
        slots.append(free.pop(free.index(min(free))))
        copy = pltpu.make_async_remote_copy(
            src_ref=src, dst_ref=dst, send_sem=ssem.at[slots[-1]], recv_sem=rsem.at[len(sent)],
            device_id=dev, device_id_type=MESH)
        copy.start()
        sent.append(copy)
        return copy

    done = [0]

    def left(n):
        for k in range(done[0], n):
            sent[k].wait_send()
            free.append(slots[k])
        done[0] = max(done[0], n)

    def local(k, src, dst):
        copy = pltpu.make_async_copy(src, dst, lsem.at[k])
        copy.start()
        return copy

    def got(*copies):
        for copy in copies:
            copy.wait_recv()

    slab = pl.ds(pl.multiple_of(c * 768, 128), 768)
    mine = pl.ds(pl.multiple_of(c * 3072, 128), 3072)
    other = pl.ds(pl.multiple_of((1 - c) * 3072, 128), 3072)
    ca, cb = pl.ds(0, GA), pl.ds(GA, 6144 - GA)
    hb = (6144 - GA) // 2
    cb0, cb1 = pl.ds(GA, hb), pl.ds(GA + hb, hb)

    def xrow(r):
        return xs.at[r, :, slab]

    def grow(xx, yy, cols):
        return gs.at[xx * 4 + yy, c, :, cols]

    t_x = send(tok, xrow(row), d_hx)
    t_op = send(tok, xrow(row), d_zp)
    t_om = send(tok, xrow(row), d_zm)
    h_x = send(hg.at[:, ca], grow(xl, y, ca), d_xp)
    h_op = send(hg.at[:, ca], grow(xl, y, ca), d_yp)
    h_om = send(hg.at[:, ca], grow(xl, y, ca), d_ym)
    w_c = send(w.at[:, other], g.at[:, mine], d_cp)
    t_c = [send(tok, xrow(row), d_cp)]
    b_op = send(hg.at[:, cb], grow(xl, y, cb), d_yp)
    b_om = send(hg.at[:, cb], grow(xl, y, cb), d_ym)
    b_x = [send(hg.at[:, cb], grow(xl, y, cb), d_xp)]
    l_t = local(0, tok, xrow(row))
    l_w = local(1, w.at[:, mine], g.at[:, mine])
    l_h = local(2, hg, gs.at[xl * 4 + y, c])
    l_p = local(3, prev, pv.at[row])

    got(t_x)
    t_pp = send(xrow(rowx), xrow(rowx), d_zp)
    t_pm = send(xrow(rowx), xrow(rowx), d_zm)
    t_c.append(send(xrow(rowx), xrow(rowx), d_cp))
    p_x = send(prev, pv.at[row], d_hx)
    got(t_op, t_om)
    t_f0 = send(xrow(zb + zm), xrow(zb + zm), d_zp)
    t_c.append(send(xrow(zb + zm), xrow(zb + zm), d_cp))
    t_c.append(send(xrow(zb + zp), xrow(zb + zp), d_cp))
    got(t_pp, t_pm)
    t_f1 = send(xrow(zbx + zp), xrow(zbx + zp), d_zm)
    t_c.append(send(xrow(zbx + zm), xrow(zbx + zm), d_cp))
    t_c.append(send(xrow(zbx + zp), xrow(zbx + zp), d_cp))
    p_op = send(prev, pv.at[row], d_zp)
    p_om = send(prev, pv.at[row], d_zm)
    got(h_x)
    h_pp = send(grow(xo, y, ca), grow(xo, y, ca), d_yp)
    h_pm = send(grow(xo, y, ca), grow(xo, y, ca), d_ym)
    got(h_op, h_om)
    h_f0 = send(grow(xl, ym, ca), grow(xl, ym, ca), d_yp)
    got(b_op, b_om)
    b_f1 = send(grow(xl, yp, cb1), grow(xl, yp, cb1), d_ym)
    b_f0 = send(grow(xl, ym, cb0), grow(xl, ym, cb0), d_yp)
    b_x.append(send(grow(xl, ym, cb), grow(xl, ym, cb), d_xp))
    got(t_f0, t_f1)
    t_c.append(send(xrow(zb + z2), xrow(zb + z2), d_cp))
    t_c.append(send(xrow(zbx + z2), xrow(zbx + z2), d_cp))
    l_t.wait()
    l_w.wait()
    got(w_c, *t_c)

    def product(lo, hi):
        def tile(i, carry):
            cols = pl.ds(pl.multiple_of(i * 256, 256), 256)
            cols2 = pl.ds(pl.multiple_of(i * 256 + 3072, 256), 256)
            part[:, cols] = jnp.dot(
                xs[...].reshape(1024, 1536),
                jnp.concatenate([g[:, cols], g[:, cols2]], axis=0),
                preferred_element_type=jnp.float32)
            return carry

        lax.fori_loop(lo // 256, hi // 256, tile, 0)

    def prow(xx, yy):
        return pl.ds(pl.multiple_of((xx * 4 + yy) * TB, TB), TB)

    def scales(tile):
        v = tile.astype(jnp.int32).astype(jnp.float32)
        return v[8:16] * (1.0 / 8192.0) * jnp.exp2(v[0:8])

    def quant(rows, c0, n, q):
        def peak(k, m):
            v = part[rows, pl.ds(pl.multiple_of(c0 + k * 128, 128), 128)]
            return jnp.maximum(m, jnp.max(jnp.abs(v.reshape(16, 8, 128)), axis=0))

        m = lax.fori_loop(0, n // 128, peak, jnp.full((8, 128), 1e-30, jnp.float32))
        m = m * (1.0 / 32766.0)
        e = jnp.floor(jnp.log2(m))
        m = jnp.ceil(m * jnp.exp2(-e) * 8192.0)
        tile = jnp.concatenate([e, m], axis=0).astype(jnp.int32).astype(jnp.int16)
        q[16] = tile
        q[33] = tile
        inv = 1.0 / scales(tile)

        def code(k, carry):
            v = part[rows, pl.ds(pl.multiple_of(c0 + k * 128, 128), 128)]
            v = (v.reshape(16, 8, 128) * inv[None]).reshape(2, 4, 16, 128)
            v = jnp.round(v).astype(jnp.int32).astype(jnp.int16)
            q[pl.ds(k * 4, 4)] = v[0]
            q[pl.ds(17 + k * 4, 4)] = v[1]
            return carry

        lax.fori_loop(0, n // 128, code, 0)

    def add(rows, c0, n, q):
        s = scales(q[16])

        def step(k, carry):
            cols = pl.ds(pl.multiple_of(c0 + k * 128, 128), 128)
            v = jnp.concatenate([q[pl.ds(k * 4, 4)], q[pl.ds(17 + k * 4, 4)]], axis=0)
            v = v.astype(jnp.int32).astype(jnp.float32).reshape(16, 8, 128) * s[None]
            part[rows, cols] = part[rows, cols] + v.reshape(TB, 128)
            return carry

        lax.fori_loop(0, n // 128, step, 0)

    def a_first(i):
        c0, n = A_PIECES[i]
        for yy in range(4):
            quant(prow(xo, yy), c0, n, ax_s.at[i, yy])
        return send(ax_s.at[i, :, pl.ds(0, 33)], ax_r.at[i, :, pl.ds(0, 33)], d_xp)

    def a_second(i, first):
        c0, n = A_PIECES[i]
        d_d = d_yp if i % 2 == 0 else d_ym
        got(first)
        for yy in range(4):
            add(prow(xl, yy), c0, n, ax_r.at[i, yy])
        a_own.append(share(c0, n))
        quant(prow(xl, y2), c0, n, ay_s.at[i, 0])
        return send(ay_s.at[i, 0, pl.ds(0, 33)], ay_r.at[i, pl.ds(0, 33)], d_d)

    def a_near(i):
        c0, n = A_PIECES[i]
        yo, d_o = (ym, d_ym) if i % 2 == 0 else (yp, d_yp)
        quant(prow(xl, yo), c0, n, ay_s.at[i, 1])
        return send_last(ay_s.at[i, 1], af_r.at[i, 0], d_o)

    own_part = pl.ds(pl.multiple_of((xl * 4 + y) * TB + c * 64, 64), 64)
    their_part = pl.ds(pl.multiple_of((xl * 4 + y) * TB + (1 - c) * 64, 64), 64)
    a_own, b_own = [], []

    def share(c0, n):
        return send(part.at[their_part, pl.ds(c0, n)], oth.at[:, pl.ds(c0, n)], d_cp)

    def send_last(qs, qr, dev):
        dev2 = (dev[0], dev[1] + 1 - 2 * c)
        return (send(qs.at[pl.ds(c * 17, 17)], qr.at[0], dev),
                send(qs.at[pl.ds((1 - c) * 17, 17)], qr.at[1], dev2))

    def a_third(i, far):
        c0, n = A_PIECES[i]
        yd, d_d = (yp, d_yp) if i % 2 == 0 else (ym, d_ym)
        got(far)
        add(prow(xl, yd), c0, n, ay_r.at[i])
        quant(prow(xl, yd), c0, n, ay_s.at[i, 2])
        return send_last(ay_s.at[i, 2], af_r.at[i, 1], d_d)

    def a_last(i, near, passed):
        c0, n = A_PIECES[i]
        got(*near, *passed, a_own[i])
        for k in range(2):
            finish(c0, n, k, [af_r.at[i, j, k] for j in range(2)])

    def b_y(i, k, rows, dev):
        c0, n = B_PIECES[i]
        quant(rows, c0, n, by_s.at[i, k])
        return send(by_s.at[i, k, pl.ds(0, 33)], by_r.at[i, k, pl.ds(0, 33)], dev)

    def b_first(i):
        return b_y(i, 0, prow(0, y2), d_yp), b_y(i, 1, prow(1, y2), d_ym)

    def b_near(i):
        return b_y(i, 2, prow(1, yp), d_yp), b_y(i, 3, prow(0, ym), d_ym)

    def b_second(i, first):
        c0, n = B_PIECES[i]
        got(first[0])
        add(prow(0, yp), c0, n, by_r.at[i, 0])
        up = b_y(i, 4, prow(0, yp), d_yp)
        got(first[1])
        add(prow(1, ym), c0, n, by_r.at[i, 1])
        down = b_y(i, 5, prow(1, ym), d_ym)
        return up, down

    def b_third(i, near, second):
        c0, n = B_PIECES[i]
        got(*near)
        add(prow(1, y), c0, n, by_r.at[i, 2])
        add(prow(0, y), c0, n, by_r.at[i, 3])
        got(*second)
        add(prow(0, y), c0, n, by_r.at[i, 4])
        add(prow(1, y), c0, n, by_r.at[i, 5])
        quant(prow(xo, y), c0, n, bx_s.at[i])
        out = send_last(bx_s.at[i], bf_r.at[i], d_xp)
        b_own.append(share(c0, n))
        return out

    def b_last(i, third):
        c0, n = B_PIECES[i]
        got(*third, b_own[i])
        for k in range(2):
            finish(c0, n, k, [bf_r.at[i, k]])

    unit_limit = active[0] * BLOCK - row * 6144

    def unit_mask(first, rows, n):
        return first + lax.broadcasted_iota(jnp.int32, (rows, n), 1) < unit_limit

    def grad(lo, hi):
        def tile(i, carry):
            cols = pl.ds(pl.multiple_of(i * GSTEP, GSTEP), GSTEP)
            v = jnp.dot(pvt[...], gs[:, :, :, cols].reshape(1024, GSTEP),
                        preferred_element_type=jnp.float32)
            g[:, cols] = jnp.where(unit_mask(i * GSTEP, 768, GSTEP), v, 0.0).astype(jnp.bfloat16)
            return carry

        lax.fori_loop(lo, hi, tile, 0)

    def finish(c0, n, k, terms):
        first = c * 3072 if k == 0 else (1 - c) * 3072
        factors = [scales(q[16]) for q in terms]

        def step(j, carry):
            at = pl.multiple_of(c0 + j * 128, 128)
            v = part[own_part, pl.ds(at, 128)] if k == 0 else oth[:, pl.ds(at, 128)]
            v = v.reshape(8, 8, 128)
            for q, s in zip(terms, factors):
                t = q[pl.ds(j * 4, 4)].astype(jnp.int32).astype(jnp.float32)
                v = v + t.reshape(8, 8, 128) * s[None]
            v = v.reshape(64, 128)
            v = v * (lax.erf(v * 0.7071067811865476) + 1.0) * 0.5
            v = jnp.where(unit_mask(first + at, 64, 128), v, 0.0)
            act[:, pl.ds(pl.multiple_of(first + at, 128), 128)] = v.astype(jnp.bfloat16)
            return carry

        lax.fori_loop(0, n // 128, step, 0)

    c_b1 = []

    def forward(k, yy):
        got(b_x[k])
        c_b1.append(send(grow(xo, yy, cb), grow(xo, yy, cb), d_cp))

    product(0, A_COLS)
    a1 = [a_first(i) for i in range(len(A_PIECES))]
    b_x.append(send(grow(xl, yp, cb), grow(xl, yp, cb), d_xp))
    got(h_pp, h_pm)
    h_f1 = send(grow(xo, yp, ca), grow(xo, yp, ca), d_ym)
    product(B_PIECES[0][0], B_PIECES[2][0])
    b1 = [b_first(0), b_first(1)]
    got(p_x)
    p_pp = send(pv.at[rowx], pv.at[rowx], d_zp)
    p_pm = send(pv.at[rowx], pv.at[rowx], d_zm)
    got(b_f1)
    b_x.append(send(grow(xl, y2, cb1), grow(xl, y2, cb1), d_xp))
    product(B_PIECES[2][0], 3072)
    b1 += [b_first(2), b_first(3)]
    got(p_op, p_om)
    p_f0 = send(pv.at[zb + zm], pv.at[zb + zm], d_zp)
    b1n = [b_near(i) for i in range(4)]
    got(p_pp, p_pm)
    p_f1 = send(pv.at[zbx + zp], pv.at[zbx + zp], d_zm)
    got(h_f0)
    got(b_f0)
    b_x.append(send(grow(xl, y2, cb0), grow(xl, y2, cb0), d_xp))
    l_h.wait()
    near_rows = pl.ds(xl * 4, 4)
    c_b0 = send(gs.at[near_rows, c, :, cb], gs.at[near_rows, c, :, cb], d_cp)
    got(h_f1)
    c_a = send(gs.at[:, c, :, ca], gs.at[:, c, :, ca], d_cp)
    n1 = len(sent)
    b2 = [b_second(0, b1[0])]
    a2 = [a_second(0, a1[0])]
    l_p.wait()
    got(p_f0, p_f1)
    pvt[...] = pv[...].reshape(1024, 768).T
    b2.append(b_second(1, b1[1]))
    left(24)
    got(c_a)
    a2.append(a_second(1, a1[1]))
    b2.append(b_second(2, b1[2]))
    b2.append(b_second(3, b1[3]))
    n2 = len(sent)
    an = [a_near(0), a_near(1)]
    left(31)
    grad(0, 3)
    forward(0, y)
    forward(1, ym)
    grad(3, 7)
    forward(2, yp)
    got(b_x[3])
    b3 = [b_third(0, b1n[0], b2[0])]
    a3 = [a_third(0, a2[0])]
    got(b_x[4])
    c_b1.append(send(grow(xo, y2, cb), grow(xo, y2, cb), d_cp))
    b3.append(b_third(1, b1n[1], b2[1]))
    a3.append(a_third(1, a2[1]))
    got(c_b0, *c_b1)
    left(n1)
    grad(7, 9)
    b3.append(b_third(2, b1n[2], b2[2]))
    grad(9, 10)
    b3.append(b_third(3, b1n[3], b2[3]))
    grad(10, 12)
    left(n2)
    b_last(0, b3[0])
    b_last(1, b3[1])
    b_last(2, b3[2])
    a_last(0, an[0], a3[0])
    a_last(1, an[1], a3[1])
    b_last(3, b3[3])
    left(len(sent))


def exchange(active_blocks, tokens, prev_tokens, hidden_grad, weight):
    bf, f32, i16 = jnp.bfloat16, jnp.float32, jnp.int16
    any_space = pl.BlockSpec(memory_space=pl.ANY)
    vmem = pl.BlockSpec(memory_space=pltpu.VMEM)
    pa, pb = len(A_PIECES), len(B_PIECES)

    def pair(shape, dtype):
        return [pltpu.VMEM(shape, dtype)] * 2

    return pl.pallas_call(
        kernel,
        out_shape=(pltpu.VMEM((64, 6144), bf), pltpu.VMEM((768, 6144), bf)),
        in_specs=[pl.BlockSpec(memory_space=pltpu.SMEM)] + [any_space] * 4,
        out_specs=(vmem, vmem),
        scratch_shapes=[
            pltpu.VMEM((8, 128, 1536), bf),
            pltpu.VMEM((8, 128, 768), bf),
            pltpu.VMEM((768, 1024), bf),
            pltpu.VMEM((8, 2, 64, 6144), bf),
            pltpu.VMEM((1024, 3072), f32),
            pltpu.VMEM((64, 3072), f32),
            *pair((pa, 4, 34, 16, 128), i16),
            pltpu.VMEM((pa, 3, 34, 16, 128), i16),
            pltpu.VMEM((pa, 34, 16, 128), i16),
            *pair((pb, 6, 34, 16, 128), i16),
            pltpu.VMEM((pb, 34, 16, 128), i16),
            pltpu.VMEM((pa, 2, 2, 17, 16, 128), i16),
            pltpu.VMEM((pb, 2, 17, 16, 128), i16),
            pltpu.SemaphoreType.DMA((N_SENDS,)),
            pltpu.SemaphoreType.DMA((N_COPIES,)),
            pltpu.SemaphoreType.DMA((4,)),
        ],
        compiler_params=pltpu.CompilerParams(
            collective_id=0, has_side_effects=True, vmem_limit_bytes=VMEM_LIMIT),
    )(active_blocks, *(pltpu.with_memory_space_constraint(a, pltpu.HBM)
                       for a in (tokens, prev_tokens, hidden_grad, weight)))


def store_kernel(act, g, act_out, g_out, sems):
    copies = [pltpu.make_async_copy(act, act_out, sems.at[4])]
    for k in range(4):
        rows = pl.ds(k * 192, 192)
        copies.append(pltpu.make_async_copy(g.at[rows], g_out.at[rows], sems.at[k]))
    for copy in copies:
        copy.start()
    for copy in copies:
        copy.wait()


def store(act, g):
    return pl.pallas_call(
        store_kernel,
        out_shape=(jax.ShapeDtypeStruct(act.shape, act.dtype), jax.ShapeDtypeStruct(g.shape, g.dtype)),
        in_specs=[pl.BlockSpec(memory_space=pltpu.VMEM)] * 2,
        out_specs=[pl.BlockSpec(memory_space=pl.ANY)] * 2,
        scratch_shapes=[pltpu.SemaphoreType.DMA((5,))],
        compiler_params=pltpu.CompilerParams(vmem_limit_bytes=12 * 1024 * 1024),
    )(act, g)


def shards(tokens, prev_tokens, hidden_grad, active_blocks, weight):
    act, grad = exchange(active_blocks, tokens, prev_tokens, hidden_grad, weight)
    return tuple(store(act, grad))


def solution(mesh):
    return jax.shard_map(
        shards,
        mesh=mesh,
        in_specs=(P("row", "col"), P("row", "col"), P("col", "row"), P(), P("col", "row")),
        out_specs=(P("col", "row"), P("col", "row")),
        check_vma=False,
    )
```

```python
import jax
import jax.numpy as jnp
from jax import lax
from jax.experimental import pallas as pl
from jax.experimental.pallas import tpu as pltpu
from jax.sharding import PartitionSpec as P

BLOCK = 3072
MESH = pl.DeviceIdType.MESH
TB = 128
A_AT = (0, 512)
B_AT = (1024, 1536, 2048, 2560)
GA = 3584
GB = 1280
GSTEP = 512
N_COPIES = 81
N_SENDS = 52
VMEM_LIMIT = 54 * 1000 * 1000


def kernel(active, tok, prev, hg, w, act, g, xs, pv, pvt, gs, part, oth,
           ax_s, ax_r, ay_s, ay_r, af_s, bp_s, bp_r, bn_s, bn_r, by_s, by_r, bx_s, af_r, bf_r,
           ssem, rsem, lsem):
    row, col = lax.axis_index("row"), lax.axis_index("col")
    z, c = lax.rem(row, 4), lax.rem(col, 2)
    half = lax.div(col, 2)
    y, xl = lax.rem(half, 4), lax.div(half, 4)
    zb, yb = row - z, xl * 8 + c
    yp, ym, y2 = lax.rem(y + 1, 4), lax.rem(y + 3, 4), lax.rem(y + 2, 4)
    zp, zm, z2 = lax.rem(z + 1, 4), lax.rem(z + 3, 4), lax.rem(z + 2, 4)
    xo = 1 - xl
    rowx = lax.rem(row + 4, 8)
    zbx = rowx - z
    d_cp = (row, col + 1 - 2 * c)
    d_xp = (row, lax.rem(col + 8, 16))
    d_yp, d_ym = (row, yb + yp * 2), (row, yb + ym * 2)
    d_hx = (rowx, col)
    d_zp, d_zm = (zb + zp, col), (zb + zm, col)

    sent, slots, free = [], [], list(range(N_SENDS))

    def send(src, dst, dev):
        slots.append(free.pop(free.index(min(free))))
        copy = pltpu.make_async_remote_copy(
            src_ref=src, dst_ref=dst, send_sem=ssem.at[slots[-1]], recv_sem=rsem.at[len(sent)],
            device_id=dev, device_id_type=MESH)
        copy.start()
        sent.append(copy)
        return copy

    done = [0]

    def left(n):
        for k in range(done[0], n):
            sent[k].wait_send()
            free.append(slots[k])
        done[0] = max(done[0], n)

    def local(k, src, dst):
        copy = pltpu.make_async_copy(src, dst, lsem.at[k])
        copy.start()
        return copy

    def got(*copies):
        for copy in copies:
            copy.wait_recv()

    slab = pl.ds(pl.multiple_of(c * 768, 128), 768)
    mine = pl.ds(pl.multiple_of(c * 3072, 128), 3072)
    other = pl.ds(pl.multiple_of((1 - c) * 3072, 128), 3072)
    ca, cb = pl.ds(0, GA), pl.ds(GA, 6144 - GA)
    cb0, cb1 = pl.ds(GA, GB), pl.ds(GA + GB, 6144 - GA - GB)

    def xrow(r):
        return xs.at[r, :, slab]

    def group(r):
        return xs.at[pl.ds(r, 4), :, slab]

    def grow(xx, yy, cols):
        return gs.at[xx * 4 + yy, c, :, cols]

    l_h = local(2, hg, gs.at[xl * 4 + y, c])
    l_t = local(0, tok, xrow(row))
    l_p = local(3, prev, pv.at[row])
    l_w = local(1, w.at[:, mine], g.at[:, mine])

    barrier = pltpu.get_barrier_semaphore()
    peers = (d_cp, d_xp, d_yp, d_ym, d_hx, d_zp, d_zm)
    for d in peers:
        pl.semaphore_signal(barrier, inc=1, device_id=d, device_id_type=MESH)
    pl.semaphore_wait(barrier, len(peers))

    l_h.wait()
    l_t.wait()
    l_p.wait()
    t_x = send(xrow(row), xrow(row), d_hx)
    t_op = send(xrow(row), xrow(row), d_zp)
    t_om = send(xrow(row), xrow(row), d_zm)
    h_x = send(grow(xl, y, ca), grow(xl, y, ca), d_xp)
    h_op = send(grow(xl, y, ca), grow(xl, y, ca), d_yp)
    h_om = send(grow(xl, y, ca), grow(xl, y, ca), d_ym)
    w_c = send(w.at[:, other], g.at[:, mine], d_cp)
    b_op = send(grow(xl, y, cb), grow(xl, y, cb), d_yp)
    b_om = send(grow(xl, y, cb), grow(xl, y, cb), d_ym)
    b_x = [send(grow(xl, y, cb), grow(xl, y, cb), d_xp)]

    got(t_x)
    t_pp = send(xrow(rowx), xrow(rowx), d_zp)
    t_pm = send(xrow(rowx), xrow(rowx), d_zm)
    p_x = send(pv.at[row], pv.at[row], d_hx)
    got(t_op, t_om)
    t_f0 = send(xrow(zb + zm), xrow(zb + zm), d_zp)
    got(t_pp, t_pm)
    t_f1 = send(xrow(zbx + zp), xrow(zbx + zp), d_zm)
    p_op = send(pv.at[row], pv.at[row], d_zp)
    p_om = send(pv.at[row], pv.at[row], d_zm)
    got(h_x)
    h_pp = send(grow(xo, y, ca), grow(xo, y, ca), d_yp)
    h_pm = send(grow(xo, y, ca), grow(xo, y, ca), d_ym)
    got(h_op, h_om)
    h_f0 = send(grow(xl, ym, ca), grow(xl, ym, ca), d_yp)
    got(b_op, b_om)
    b_f1 = send(grow(xl, yp, cb1), grow(xl, yp, cb1), d_ym)
    b_f0 = send(grow(xl, ym, cb0), grow(xl, ym, cb0), d_yp)
    b_x.append(send(grow(xl, ym, cb), grow(xl, ym, cb), d_xp))
    got(t_f0, t_f1)
    t_c = [send(group(zb), group(zb), d_cp), send(group(zbx), group(zbx), d_cp)]
    l_w.wait()
    got(w_c, *t_c)

    def product(lo, hi):
        def tile(i, carry):
            cols = pl.ds(pl.multiple_of(i * 256, 256), 256)
            cols2 = pl.ds(pl.multiple_of(i * 256 + 3072, 256), 256)
            part[:, cols] = jnp.dot(
                xs[...].reshape(1024, 1536),
                jnp.concatenate([g[:, cols], g[:, cols2]], axis=0),
                preferred_element_type=jnp.float32)
            return carry

        lax.fori_loop(lo // 256, hi // 256, tile, 0)

    def prow(xx, yy):
        return pl.ds(pl.multiple_of((xx * 4 + yy) * TB, TB), TB)

    N = 512

    def scales(tile):
        v = tile.astype(jnp.int32).astype(jnp.float32)
        return v[8:16] * (1.0 / 8192.0) * jnp.exp2(v[0:8])

    def lanes(c0, k):
        return pl.ds(pl.multiple_of(c0 + k * 128, 128), 128)

    def common(blocks):
        m = jnp.full((8, 128), 1e-30, jnp.float32)
        for rows, c0 in blocks:
            def peak(k, m, rows=rows, c0=c0):
                return jnp.maximum(m, jnp.max(jnp.abs(part[rows, lanes(c0, k)].reshape(16, 8, 128)), axis=0))

            m = lax.fori_loop(0, N // 128, peak, m)
        m = m * (1.0 / 32766.0)
        e = jnp.floor(jnp.log2(m))
        m = jnp.ceil(m * jnp.exp2(-e) * 8192.0)
        tile = jnp.concatenate([e, m], axis=0).astype(jnp.int32).astype(jnp.int16)
        return tile, 1.0 / scales(tile)

    def code(rows, c0, q, inv, first=0, second=16):
        def step(k, carry):
            v = part[rows, lanes(c0, k)].reshape(16, 8, 128) * inv[None]
            v = jnp.round(v.reshape(2, 4, 16, 128)).astype(jnp.int32).astype(jnp.int16)
            q[pl.ds(first + k * 4, 4)] = v[0]
            q[pl.ds(second + k * 4, 4)] = v[1]
            return carry

        lax.fori_loop(0, N // 128, step, 0)

    def add(rows, c0, q, s, first=0):
        def step(k, carry):
            v = jnp.concatenate([q[pl.ds(first + k * 4, 4)], q[pl.ds(first + 16 + k * 4, 4)]], axis=0)
            v = v.astype(jnp.int32).astype(jnp.float32).reshape(16, 8, 128) * s[None]
            part[rows, lanes(c0, k)] = part[rows, lanes(c0, k)] + v.reshape(TB, 128)
            return carry

        lax.fori_loop(0, N // 128, step, 0)

    def post(rows, c0, qs, qr, dev):
        tile, inv = common([(rows, c0)])
        code(rows, c0, qs, inv)
        qs[32] = tile
        return send(qs, qr, dev)

    def post_last(rows, c0, qs, qr, dev):
        tile, inv = common([(rows, c0)])
        code(rows, c0, qs, inv, 0, 17)
        qs[16] = tile
        qs[33] = tile
        dev2 = (dev[0], dev[1] + 1 - 2 * c)
        return (send(qs.at[pl.ds(c * 17, 17)], qr.at[0], dev),
                send(qs.at[pl.ds((1 - c) * 17, 17)], qr.at[1], dev2))

    own_part = pl.ds(pl.multiple_of((xl * 4 + y) * TB + c * 64, 64), 64)
    their_part = pl.ds(pl.multiple_of((xl * 4 + y) * TB + (1 - c) * 64, 64), 64)
    a_own, b_own = [], []

    def share(c0):
        return send(part.at[their_part, pl.ds(c0, N)], oth.at[:, pl.ds(c0, N)], d_cp)

    def a_first(i):
        blocks = [(prow(xo, yy), A_AT[i]) for yy in range(4)]
        tile, inv = common(blocks)
        for yy, (rows, c0) in enumerate(blocks):
            code(rows, c0, ax_s.at[i], inv, yy * 32, yy * 32 + 16)
        ax_s[i, 128] = tile
        return send(ax_s.at[i], ax_r.at[i], d_xp)

    def a_second(i, first):
        c0 = A_AT[i]
        got(first)
        s = scales(ax_r[i, 128])
        for yy in range(4):
            add(prow(xl, yy), c0, ax_r.at[i], s, yy * 32)
        a_own.append(share(c0))
        return post(prow(xl, y2), c0, ay_s.at[i], ay_r.at[i], d_yp if i % 2 == 0 else d_ym)

    def a_near(i):
        yo, d_o = (ym, d_ym) if i % 2 == 0 else (yp, d_yp)
        return post_last(prow(xl, yo), A_AT[i], af_s.at[i, 0], af_r.at[i, 0], d_o)

    def a_third(i, far):
        yd, d_d = (yp, d_yp) if i % 2 == 0 else (ym, d_ym)
        got(far)
        add(prow(xl, yd), A_AT[i], ay_r.at[i], scales(ay_r[i, 32]))
        return post_last(prow(xl, yd), A_AT[i], af_s.at[i, 1], af_r.at[i, 1], d_d)

    def a_last(i, near, passed):
        got(*near, *passed, a_own[i])
        for k in range(2):
            finish(A_AT[i], k, [af_r.at[i, j, k] for j in range(2)])

    def b_first(p):
        out = []
        for k, far_rows, near_rows, dev in ((0, prow(0, y2), prow(1, yp), d_yp), (1, prow(1, y2), prow(0, ym), d_ym)):
            at = [B_AT[2 * p], B_AT[2 * p + 1]]
            tile, inv = common([(r, c0) for r in (far_rows, near_rows) for c0 in at])
            for j in range(2):
                code(far_rows, at[j], bp_s.at[p, k], inv, j * 32, j * 32 + 16)
                code(near_rows, at[j], bn_s.at[p, k], inv, j * 32, j * 32 + 16)
            bp_s[p, k, 64] = tile
            out.append(send(bp_s.at[p, k], bp_r.at[p, k], dev))
        return out

    def b_near(p):
        return [send(bn_s.at[p, k], bn_r.at[p, k], dev) for k, dev in ((0, d_yp), (1, d_ym))]

    def b_second(i, first):
        p, j, out = i // 2, i % 2, []
        for k, rows, dev in ((0, prow(0, yp), d_yp), (1, prow(1, ym), d_ym)):
            if j == 0:
                got(first[k])
            add(rows, B_AT[i], bp_r.at[p, k], scales(bp_r[p, k, 64]), j * 32)
            out.append(post(rows, B_AT[i], by_s.at[i, k], by_r.at[i, k], dev))
        return out

    def b_third(i, near, second):
        p, j, c0 = i // 2, i % 2, B_AT[i]
        if j == 0:
            got(*near)
        for k, rows in ((0, prow(1, y)), (1, prow(0, y))):
            add(rows, c0, bn_r.at[p, k], scales(bp_r[p, k, 64]), j * 32)
        got(*second)
        for k, rows in ((0, prow(0, y)), (1, prow(1, y))):
            add(rows, c0, by_r.at[i, k], scales(by_r[i, k, 32]))
        out = post_last(prow(xo, y), c0, bx_s.at[i], bf_r.at[i], d_xp)
        b_own.append(share(c0))
        return out

    def b_last(i, third):
        got(*third, b_own[i])
        for k in range(2):
            finish(B_AT[i], k, [bf_r.at[i, k]])

    unit_limit = active[0] * BLOCK - row * 6144

    def unit_mask(first, rows, n):
        return first + lax.broadcasted_iota(jnp.int32, (rows, n), 1) < unit_limit

    def grad(lo, hi):
        def tile(i, carry):
            cols = pl.ds(pl.multiple_of(i * GSTEP, GSTEP), GSTEP)
            v = jnp.dot(pvt[...], gs[:, :, :, cols].reshape(1024, GSTEP),
                        preferred_element_type=jnp.float32)
            g[:, cols] = jnp.where(unit_mask(i * GSTEP, 768, GSTEP), v, 0.0).astype(jnp.bfloat16)
            return carry

        lax.fori_loop(lo, hi, tile, 0)

    def finish(c0, k, terms):
        first = c * 3072 if k == 0 else (1 - c) * 3072
        factors = [scales(q[16]) for q in terms]

        def step(j, carry):
            at = pl.multiple_of(c0 + j * 128, 128)
            v = part[own_part, pl.ds(at, 128)] if k == 0 else oth[:, pl.ds(at, 128)]
            v = v.reshape(8, 8, 128)
            for q, s in zip(terms, factors):
                t = q[pl.ds(j * 4, 4)].astype(jnp.int32).astype(jnp.float32)
                v = v + t.reshape(8, 8, 128) * s[None]
            v = v.reshape(64, 128)
            v = v * (lax.erf(v * 0.7071067811865476) + 1.0) * 0.5
            v = jnp.where(unit_mask(first + at, 64, 128), v, 0.0)
            act[:, pl.ds(pl.multiple_of(first + at, 128), 128)] = v.astype(jnp.bfloat16)
            return carry

        lax.fori_loop(0, N // 128, step, 0)

    c_b1 = []

    def forward(k, yy):
        got(b_x[k])
        c_b1.append(send(grow(xo, yy, cb), grow(xo, yy, cb), d_cp))

    product(0, 1024)
    a1 = [a_first(i) for i in range(2)]
    b_x.append(send(grow(xl, yp, cb), grow(xl, yp, cb), d_xp))
    got(h_pp, h_pm)
    h_f1 = send(grow(xo, yp, ca), grow(xo, yp, ca), d_ym)
    product(1024, 2048)
    b1 = [b_first(0)]
    got(p_x)
    p_pp = send(pv.at[rowx], pv.at[rowx], d_zp)
    p_pm = send(pv.at[rowx], pv.at[rowx], d_zm)
    got(b_f1)
    b_x.append(send(grow(xl, y2, cb1), grow(xl, y2, cb1), d_xp))
    product(2048, 3072)
    b1.append(b_first(1))
    got(p_op, p_om)
    p_f0 = send(pv.at[zb + zm], pv.at[zb + zm], d_zp)
    b1n = [b_near(0)]
    got(p_pp, p_pm)
    p_f1 = send(pv.at[zbx + zp], pv.at[zbx + zp], d_zm)
    got(h_f0)
    got(b_f0)
    b_x.append(send(grow(xl, y2, cb0), grow(xl, y2, cb0), d_xp))
    near_rows = pl.ds(xl * 4, 4)
    c_b0 = send(gs.at[near_rows, c, :, cb], gs.at[near_rows, c, :, cb], d_cp)
    got(h_f1)
    c_a = send(gs.at[:, c, :, ca], gs.at[:, c, :, ca], d_cp)
    n1 = len(sent)
    b2 = [b_second(0, b1[0])]
    b1n.append(b_near(1))
    a2 = [a_second(0, a1[0])]
    got(p_f0, p_f1)
    pvt[...] = pv[...].reshape(1024, 768).T
    b2.append(b_second(1, b1[0]))
    left(19)
    b2.append(b_second(2, b1[1]))
    b2.append(b_second(3, b1[1]))
    n2 = len(sent)
    got(c_a)
    grad(0, 2)
    a2.append(a_second(1, a1[1]))
    an = [a_near(0), a_near(1)]
    forward(0, y)
    forward(1, ym)
    grad(2, 3)
    b3 = [b_third(0, b1n[0], b2[0])]
    left(24)
    grad(3, 5)
    forward(2, yp)
    a3 = [a_third(0, a2[0])]
    grad(5, 6)
    b3.append(b_third(1, b1n[0], b2[1]))
    got(b_x[3], b_x[4])
    c_b1.append(send(grow(xo, y2, cb), grow(xo, y2, cb), d_cp))
    b3.append(b_third(2, b1n[1], b2[2]))
    left(n1)
    got(c_b0, *c_b1)
    grad(6, 8)
    a3.append(a_third(1, a2[1]))
    b3.append(b_third(3, b1n[1], b2[3]))
    grad(8, 12)
    left(n2)
    b_last(0, b3[0])
    b_last(1, b3[1])
    b_last(2, b3[2])
    b_last(3, b3[3])
    a_last(0, an[0], a3[0])
    a_last(1, an[1], a3[1])
    left(len(sent))


def exchange(active_blocks, tokens, prev_tokens, hidden_grad, weight):
    bf, f32, i16 = jnp.bfloat16, jnp.float32, jnp.int16
    any_space = pl.BlockSpec(memory_space=pl.ANY)
    vmem = pl.BlockSpec(memory_space=pltpu.VMEM)
    pa, pb = len(A_AT), len(B_AT)

    def pair(shape, dtype):
        return [pltpu.VMEM(shape, dtype)] * 2

    return pl.pallas_call(
        kernel,
        out_shape=(pltpu.VMEM((64, 6144), bf), pltpu.VMEM((768, 6144), bf)),
        in_specs=[pl.BlockSpec(memory_space=pltpu.SMEM)] + [any_space] * 4,
        out_specs=(vmem, vmem),
        scratch_shapes=[
            pltpu.VMEM((8, 128, 1536), bf),
            pltpu.VMEM((8, 128, 768), bf),
            pltpu.VMEM((768, 1024), bf),
            pltpu.VMEM((8, 2, 64, 6144), bf),
            pltpu.VMEM((1024, 3072), f32),
            pltpu.VMEM((64, 3072), f32),
            *pair((pa, 129, 16, 128), i16),
            *pair((pa, 33, 16, 128), i16),
            pltpu.VMEM((pa, 2, 34, 16, 128), i16),
            *pair((pb // 2, 2, 65, 16, 128), i16),
            *pair((pb // 2, 2, 64, 16, 128), i16),
            *pair((pb, 2, 33, 16, 128), i16),
            pltpu.VMEM((pb, 34, 16, 128), i16),
            pltpu.VMEM((pa, 2, 2, 17, 16, 128), i16),
            pltpu.VMEM((pb, 2, 17, 16, 128), i16),
            pltpu.SemaphoreType.DMA((N_SENDS,)),
            pltpu.SemaphoreType.DMA((N_COPIES,)),
            pltpu.SemaphoreType.DMA((4,)),
        ],
        compiler_params=pltpu.CompilerParams(
            collective_id=0, has_side_effects=True, vmem_limit_bytes=VMEM_LIMIT),
    )(active_blocks, *(pltpu.with_memory_space_constraint(a, pltpu.HBM)
                       for a in (tokens, prev_tokens, hidden_grad, weight)))


def store_kernel(act, g, act_out, g_out, sems):
    copies = [pltpu.make_async_copy(act, act_out, sems.at[8])]
    for k in range(8):
        rows = pl.ds(k * 96, 96)
        copies.append(pltpu.make_async_copy(g.at[rows], g_out.at[rows], sems.at[k]))
    for copy in copies:
        copy.start()
    for copy in copies:
        copy.wait()


def store(act, g):
    return pl.pallas_call(
        store_kernel,
        out_shape=(jax.ShapeDtypeStruct(act.shape, act.dtype), jax.ShapeDtypeStruct(g.shape, g.dtype)),
        in_specs=[pl.BlockSpec(memory_space=pltpu.VMEM)] * 2,
        out_specs=[pl.BlockSpec(memory_space=pl.ANY)] * 2,
        scratch_shapes=[pltpu.SemaphoreType.DMA((9,))],
        compiler_params=pltpu.CompilerParams(vmem_limit_bytes=12 * 1024 * 1024),
    )(act, g)


def shards(tokens, prev_tokens, hidden_grad, active_blocks, weight):
    act, grad = exchange(active_blocks, tokens, prev_tokens, hidden_grad, weight)
    return tuple(store(act, grad))


def solution(mesh):
    return jax.shard_map(
        shards,
        mesh=mesh,
        in_specs=(P("row", "col"), P("row", "col"), P("col", "row"), P(), P("col", "row")),
        out_specs=(P("col", "row"), P("col", "row")),
        check_vma=False,
    )
```

```python
import jax
import jax.numpy as jnp
from jax import lax
from jax.experimental import pallas as pl
from jax.experimental.pallas import tpu as pltpu
from jax.sharding import PartitionSpec as P

BLOCK = 3072
MESH = pl.DeviceIdType.MESH
TB = 128
A_AT = (0, 512)
B_AT = (1024, 1536, 2048, 2560)
GA = 3584
GB = 1280
GSTEP = 512
N_COPIES = 81
N_SENDS = 51
VMEM_LIMIT = 54 * 1000 * 1000


def kernel(active, tok, prev, hg, w, act, g, xs, pv, pvt, gs, part, oth,
           ax_s, ax_r, ay_s, ay_r, af_s, bp_s, bp_r, bn_s, bn_r, by_s, by_r, bx_s, af_r, bf_r,
           ssem, rsem, lsem):
    row, col = lax.axis_index("row"), lax.axis_index("col")
    z, c = lax.rem(row, 4), lax.rem(col, 2)
    half = lax.div(col, 2)
    y, xl = lax.rem(half, 4), lax.div(half, 4)
    zb, yb = row - z, xl * 8 + c
    yp, ym, y2 = lax.rem(y + 1, 4), lax.rem(y + 3, 4), lax.rem(y + 2, 4)
    zp, zm, z2 = lax.rem(z + 1, 4), lax.rem(z + 3, 4), lax.rem(z + 2, 4)
    xo = 1 - xl
    rowx = lax.rem(row + 4, 8)
    zbx = rowx - z
    d_cp = (row, col + 1 - 2 * c)
    d_xp = (row, lax.rem(col + 8, 16))
    d_yp, d_ym = (row, yb + yp * 2), (row, yb + ym * 2)
    d_hx = (rowx, col)
    d_zp, d_zm = (zb + zp, col), (zb + zm, col)

    sent, slots, free = [], [], list(range(N_SENDS))

    def send(src, dst, dev):
        slots.append(free.pop(free.index(min(free))))
        copy = pltpu.make_async_remote_copy(
            src_ref=src, dst_ref=dst, send_sem=ssem.at[slots[-1]], recv_sem=rsem.at[len(sent)],
            device_id=dev, device_id_type=MESH)
        copy.start()
        sent.append(copy)
        return copy

    done = [0]

    def left(n):
        for k in range(done[0], n):
            sent[k].wait_send()
            free.append(slots[k])
        done[0] = max(done[0], n)

    def local(k, src, dst):
        copy = pltpu.make_async_copy(src, dst, lsem.at[k])
        copy.start()
        return copy

    def got(*copies):
        for copy in copies:
            copy.wait_recv()

    slab = pl.ds(pl.multiple_of(c * 768, 128), 768)
    mine = pl.ds(pl.multiple_of(c * 3072, 128), 3072)
    other = pl.ds(pl.multiple_of((1 - c) * 3072, 128), 3072)
    ca, cb = pl.ds(0, GA), pl.ds(GA, 6144 - GA)
    cb0, cb1 = pl.ds(GA, GB), pl.ds(GA + GB, 6144 - GA - GB)

    def xrow(r):
        return xs.at[r, :, slab]

    def group(r):
        return xs.at[pl.ds(r, 4), :, slab]

    def grow(xx, yy, cols):
        return gs.at[xx * 4 + yy, c, :, cols]

    l_h = local(2, hg, gs.at[xl * 4 + y, c])
    l_t = local(0, tok, xrow(row))
    l_p = local(3, prev, pv.at[row])
    l_w = local(1, w.at[:, mine], g.at[:, mine])

    barrier = pltpu.get_barrier_semaphore()
    peers = (d_cp, d_xp, d_yp, d_ym, d_hx, d_zp, d_zm)
    for d in peers:
        pl.semaphore_signal(barrier, inc=1, device_id=d, device_id_type=MESH)
    pl.semaphore_wait(barrier, len(peers))

    l_h.wait()
    l_t.wait()
    l_p.wait()
    t_x = send(xrow(row), xrow(row), d_hx)
    t_op = send(xrow(row), xrow(row), d_zp)
    t_om = send(xrow(row), xrow(row), d_zm)
    h_x = send(grow(xl, y, ca), grow(xl, y, ca), d_xp)
    h_op = send(grow(xl, y, ca), grow(xl, y, ca), d_yp)
    h_om = send(grow(xl, y, ca), grow(xl, y, ca), d_ym)
    w_c = send(w.at[:, other], g.at[:, mine], d_cp)
    b_op = send(grow(xl, y, cb), grow(xl, y, cb), d_yp)
    b_om = send(grow(xl, y, cb), grow(xl, y, cb), d_ym)
    b_x = [send(grow(xl, y, cb), grow(xl, y, cb), d_xp)]

    got(t_x)
    t_pp = send(xrow(rowx), xrow(rowx), d_zp)
    t_pm = send(xrow(rowx), xrow(rowx), d_zm)
    p_x = send(pv.at[row], pv.at[row], d_hx)
    got(t_op, t_om)
    t_f0 = send(xrow(zb + zm), xrow(zb + zm), d_zp)
    got(t_pp, t_pm)
    t_f1 = send(xrow(zbx + zp), xrow(zbx + zp), d_zm)
    p_op = send(pv.at[row], pv.at[row], d_zp)
    p_om = send(pv.at[row], pv.at[row], d_zm)
    got(h_x)
    h_pp = send(grow(xo, y, ca), grow(xo, y, ca), d_yp)
    h_pm = send(grow(xo, y, ca), grow(xo, y, ca), d_ym)
    got(h_op, h_om)
    h_f0 = send(grow(xl, ym, ca), grow(xl, ym, ca), d_yp)
    got(b_op, b_om)
    b_f1 = send(grow(xl, yp, cb1), grow(xl, yp, cb1), d_ym)
    b_f0 = send(grow(xl, ym, cb0), grow(xl, ym, cb0), d_yp)
    b_x.append(send(grow(xl, ym, cb), grow(xl, ym, cb), d_xp))
    got(t_f0, t_f1)
    t_c = [send(group(zb), group(zb), d_cp), send(group(zbx), group(zbx), d_cp)]
    l_w.wait()
    got(w_c, *t_c)

    def product(lo, hi):
        def tile(i, carry):
            cols = pl.ds(pl.multiple_of(i * 256, 256), 256)
            cols2 = pl.ds(pl.multiple_of(i * 256 + 3072, 256), 256)
            part[:, cols] = jnp.dot(
                xs[...].reshape(1024, 1536),
                jnp.concatenate([g[:, cols], g[:, cols2]], axis=0),
                preferred_element_type=jnp.float32)
            return carry

        lax.fori_loop(lo // 256, hi // 256, tile, 0)

    def prow(xx, yy):
        return pl.ds(pl.multiple_of((xx * 4 + yy) * TB, TB), TB)

    N = 512

    def scales(tile):
        v = tile.astype(jnp.int32).astype(jnp.float32)
        return v[8:16] * (1.0 / 8192.0) * jnp.exp2(v[0:8])

    def lanes(c0, k):
        return pl.ds(pl.multiple_of(c0 + k * 128, 128), 128)

    def common(blocks):
        m = jnp.full((8, 128), 1e-30, jnp.float32)
        for rows, c0 in blocks:
            def peak(k, m, rows=rows, c0=c0):
                return jnp.maximum(m, jnp.max(jnp.abs(part[rows, lanes(c0, k)].reshape(16, 8, 128)), axis=0))

            m = lax.fori_loop(0, N // 128, peak, m)
        m = m * (1.0 / 32766.0)
        e = jnp.floor(jnp.log2(m))
        m = jnp.ceil(m * jnp.exp2(-e) * 8192.0)
        tile = jnp.concatenate([e, m], axis=0).astype(jnp.int32).astype(jnp.int16)
        return tile, 1.0 / scales(tile)

    def code(rows, c0, q, inv, first=0, second=16):
        def step(k, carry):
            v = part[rows, lanes(c0, k)].reshape(16, 8, 128) * inv[None]
            v = jnp.round(v.reshape(2, 4, 16, 128)).astype(jnp.int32).astype(jnp.int16)
            q[pl.ds(first + k * 4, 4)] = v[0]
            q[pl.ds(second + k * 4, 4)] = v[1]
            return carry

        lax.fori_loop(0, N // 128, step, 0)

    def add(rows, c0, q, s, first=0):
        def step(k, carry):
            v = jnp.concatenate([q[pl.ds(first + k * 4, 4)], q[pl.ds(first + 16 + k * 4, 4)]], axis=0)
            v = v.astype(jnp.int32).astype(jnp.float32).reshape(16, 8, 128) * s[None]
            part[rows, lanes(c0, k)] = part[rows, lanes(c0, k)] + v.reshape(TB, 128)
            return carry

        lax.fori_loop(0, N // 128, step, 0)

    def post(rows, c0, qs, qr, dev):
        tile, inv = common([(rows, c0)])
        code(rows, c0, qs, inv)
        qs[32] = tile
        return send(qs, qr, dev)

    def post_last(rows, c0, qs, qr, dev):
        tile, inv = common([(rows, c0)])
        code(rows, c0, qs, inv, 0, 17)
        qs[16] = tile
        qs[33] = tile
        dev2 = (dev[0], dev[1] + 1 - 2 * c)
        return (send(qs.at[pl.ds(c * 17, 17)], qr.at[0], dev),
                send(qs.at[pl.ds((1 - c) * 17, 17)], qr.at[1], dev2))

    own_part = pl.ds(pl.multiple_of((xl * 4 + y) * TB + c * 64, 64), 64)
    their_part = pl.ds(pl.multiple_of((xl * 4 + y) * TB + (1 - c) * 64, 64), 64)
    a_own, b_own = [], []

    def share(c0):
        return send(part.at[their_part, pl.ds(c0, N)], oth.at[:, pl.ds(c0, N)], d_cp)

    def a_first(i):
        blocks = [(prow(xo, yy), A_AT[i]) for yy in range(4)]
        tile, inv = common(blocks)
        for yy, (rows, c0) in enumerate(blocks):
            code(rows, c0, ax_s.at[i], inv, yy * 32, yy * 32 + 16)
        ax_s[i, 128] = tile
        return send(ax_s.at[i], ax_r.at[i], d_xp)

    def a_second(i, first):
        c0 = A_AT[i]
        got(first)
        s = scales(ax_r[i, 128])
        for yy in range(4):
            add(prow(xl, yy), c0, ax_r.at[i], s, yy * 32)
        a_own.append(share(c0))
        return post(prow(xl, y2), c0, ay_s.at[i], ay_r.at[i], d_yp if i % 2 == 0 else d_ym)

    def a_near(i):
        yo, d_o = (ym, d_ym) if i % 2 == 0 else (yp, d_yp)
        return post_last(prow(xl, yo), A_AT[i], af_s.at[i, 0], af_r.at[i, 0], d_o)

    def a_third(i, far):
        yd, d_d = (yp, d_yp) if i % 2 == 0 else (ym, d_ym)
        got(far)
        add(prow(xl, yd), A_AT[i], ay_r.at[i], scales(ay_r[i, 32]))
        return post_last(prow(xl, yd), A_AT[i], af_s.at[i, 1], af_r.at[i, 1], d_d)

    def a_last(i, near, passed):
        got(*near, *passed, a_own[i])
        for k in range(2):
            finish(A_AT[i], k, [af_r.at[i, j, k] for j in range(2)])

    def b_first(p):
        out = []
        for k, far_rows, near_rows, dev in ((0, prow(0, y2), prow(1, yp), d_yp), (1, prow(1, y2), prow(0, ym), d_ym)):
            at = [B_AT[2 * p], B_AT[2 * p + 1]]
            tile, inv = common([(r, c0) for r in (far_rows, near_rows) for c0 in at])
            for j in range(2):
                code(far_rows, at[j], bp_s.at[p, k], inv, j * 32, j * 32 + 16)
                code(near_rows, at[j], bn_s.at[p, k], inv, j * 32, j * 32 + 16)
            bp_s[p, k, 64] = tile
            out.append(send(bp_s.at[p, k], bp_r.at[p, k], dev))
        return out

    def b_near(p):
        return [send(bn_s.at[p, k], bn_r.at[p, k], dev) for k, dev in ((0, d_yp), (1, d_ym))]

    def b_second(i, first):
        p, j, out = i // 2, i % 2, []
        for k, rows, dev in ((0, prow(0, yp), d_yp), (1, prow(1, ym), d_ym)):
            if j == 0:
                got(first[k])
            add(rows, B_AT[i], bp_r.at[p, k], scales(bp_r[p, k, 64]), j * 32)
            out.append(post(rows, B_AT[i], by_s.at[i, k], by_r.at[i, k], dev))
        return out

    def b_third(i, near, second):
        p, j, c0 = i // 2, i % 2, B_AT[i]
        if j == 0:
            got(*near)
        for k, rows in ((0, prow(1, y)), (1, prow(0, y))):
            add(rows, c0, bn_r.at[p, k], scales(bp_r[p, k, 64]), j * 32)
        got(*second)
        for k, rows in ((0, prow(0, y)), (1, prow(1, y))):
            add(rows, c0, by_r.at[i, k], scales(by_r[i, k, 32]))
        out = post_last(prow(xo, y), c0, bx_s.at[i], bf_r.at[i], d_xp)
        b_own.append(share(c0))
        return out

    def b_last(i, third):
        got(*third, b_own[i])
        for k in range(2):
            finish(B_AT[i], k, [bf_r.at[i, k]])

    unit_limit = active[0] * BLOCK - row * 6144

    def unit_mask(first, rows, n):
        return first + lax.broadcasted_iota(jnp.int32, (rows, n), 1) < unit_limit

    def grad(lo, hi):
        def tile(i, carry):
            cols = pl.ds(pl.multiple_of(i * GSTEP, GSTEP), GSTEP)
            v = jnp.dot(pvt[...], gs[:, :, :, cols].reshape(1024, GSTEP),
                        preferred_element_type=jnp.float32)
            g[:, cols] = jnp.where(unit_mask(i * GSTEP, 768, GSTEP), v, 0.0).astype(jnp.bfloat16)
            return carry

        lax.fori_loop(lo, hi, tile, 0)

    def finish(c0, k, terms):
        first = c * 3072 if k == 0 else (1 - c) * 3072
        factors = [scales(q[16]) for q in terms]

        def step(j, carry):
            at = pl.multiple_of(c0 + j * 128, 128)
            v = part[own_part, pl.ds(at, 128)] if k == 0 else oth[:, pl.ds(at, 128)]
            v = v.reshape(8, 8, 128)
            for q, s in zip(terms, factors):
                t = q[pl.ds(j * 4, 4)].astype(jnp.int32).astype(jnp.float32)
                v = v + t.reshape(8, 8, 128) * s[None]
            v = v.reshape(64, 128)
            v = v * (lax.erf(v * 0.7071067811865476) + 1.0) * 0.5
            v = jnp.where(unit_mask(first + at, 64, 128), v, 0.0)
            act[:, pl.ds(pl.multiple_of(first + at, 128), 128)] = v.astype(jnp.bfloat16)
            return carry

        lax.fori_loop(0, N // 128, step, 0)

    c_b1 = []

    def forward(k, yy):
        got(b_x[k])
        c_b1.append(send(grow(xo, yy, cb), grow(xo, yy, cb), d_cp))

    product(0, 1024)
    a1 = [a_first(i) for i in range(2)]
    b_x.append(send(grow(xl, yp, cb), grow(xl, yp, cb), d_xp))
    got(h_pp, h_pm)
    h_f1 = send(grow(xo, yp, ca), grow(xo, yp, ca), d_ym)
    product(1024, 2048)
    b1 = [b_first(0)]
    got(p_x)
    p_pp = send(pv.at[rowx], pv.at[rowx], d_zp)
    p_pm = send(pv.at[rowx], pv.at[rowx], d_zm)
    got(b_f1)
    b_x.append(send(grow(xl, y2, cb1), grow(xl, y2, cb1), d_xp))
    product(2048, 3072)
    b1.append(b_first(1))
    got(p_op, p_om)
    p_f0 = send(pv.at[zb + zm], pv.at[zb + zm], d_zp)
    b1n = [b_near(0)]
    got(p_pp, p_pm)
    p_f1 = send(pv.at[zbx + zp], pv.at[zbx + zp], d_zm)
    got(h_f0)
    got(b_f0)
    b_x.append(send(grow(xl, y2, cb0), grow(xl, y2, cb0), d_xp))
    near_rows = pl.ds(xl * 4, 4)
    c_b0 = send(gs.at[near_rows, c, :, cb], gs.at[near_rows, c, :, cb], d_cp)
    got(h_f1)
    c_a = send(gs.at[:, c, :, ca], gs.at[:, c, :, ca], d_cp)
    n1 = len(sent)
    b2 = [b_second(0, b1[0])]
    b1n.append(b_near(1))
    a2 = [a_second(0, a1[0])]
    got(p_f0, p_f1)
    pvt[...] = pv[...].reshape(1024, 768).T
    b2.append(b_second(1, b1[0]))
    left(19)
    b2.append(b_second(2, b1[1]))
    b2.append(b_second(3, b1[1]))
    n2 = len(sent)
    got(c_a)
    grad(0, 2)
    a2.append(a_second(1, a1[1]))
    an = [a_near(0), a_near(1)]
    forward(0, y)
    forward(1, ym)
    grad(2, 3)
    b3 = [b_third(0, b1n[0], b2[0])]
    left(24)
    grad(3, 5)
    forward(2, yp)
    grad(5, 6)
    got(b_x[3], b_x[4])
    c_b1.append(send(grow(xo, y2, cb), grow(xo, y2, cb), d_cp))
    a3 = [a_third(0, a2[0])]
    b3.append(b_third(1, b1n[0], b2[1]))
    left(n1)
    got(c_b0, *c_b1)
    grad(6, 8)
    b3.append(b_third(2, b1n[1], b2[2]))
    grad(8, 10)
    b3.append(b_third(3, b1n[1], b2[3]))
    a3.append(a_third(1, a2[1]))
    grad(10, 12)
    left(n2)
    b_last(0, b3[0])
    b_last(1, b3[1])
    b_last(2, b3[2])
    a_last(0, an[0], a3[0])
    a_last(1, an[1], a3[1])
    b_last(3, b3[3])
    left(len(sent))


def exchange(active_blocks, tokens, prev_tokens, hidden_grad, weight):
    bf, f32, i16 = jnp.bfloat16, jnp.float32, jnp.int16
    any_space = pl.BlockSpec(memory_space=pl.ANY)
    vmem = pl.BlockSpec(memory_space=pltpu.VMEM)
    pa, pb = len(A_AT), len(B_AT)

    def pair(shape, dtype):
        return [pltpu.VMEM(shape, dtype)] * 2

    return pl.pallas_call(
        kernel,
        out_shape=(pltpu.VMEM((64, 6144), bf), pltpu.VMEM((768, 6144), bf)),
        in_specs=[pl.BlockSpec(memory_space=pltpu.SMEM)] + [any_space] * 4,
        out_specs=(vmem, vmem),
        scratch_shapes=[
            pltpu.VMEM((8, 128, 1536), bf),
            pltpu.VMEM((8, 128, 768), bf),
            pltpu.VMEM((768, 1024), bf),
            pltpu.VMEM((8, 2, 64, 6144), bf),
            pltpu.VMEM((1024, 3072), f32),
            pltpu.VMEM((64, 3072), f32),
            *pair((pa, 129, 16, 128), i16),
            *pair((pa, 33, 16, 128), i16),
            pltpu.VMEM((pa, 2, 34, 16, 128), i16),
            *pair((pb // 2, 2, 65, 16, 128), i16),
            *pair((pb // 2, 2, 64, 16, 128), i16),
            *pair((pb, 2, 33, 16, 128), i16),
            pltpu.VMEM((pb, 34, 16, 128), i16),
            pltpu.VMEM((pa, 2, 2, 17, 16, 128), i16),
            pltpu.VMEM((pb, 2, 17, 16, 128), i16),
            pltpu.SemaphoreType.DMA((N_SENDS,)),
            pltpu.SemaphoreType.DMA((N_COPIES,)),
            pltpu.SemaphoreType.DMA((4,)),
        ],
        compiler_params=pltpu.CompilerParams(
            collective_id=0, has_side_effects=True, vmem_limit_bytes=VMEM_LIMIT),
    )(active_blocks, *(pltpu.with_memory_space_constraint(a, pltpu.HBM)
                       for a in (tokens, prev_tokens, hidden_grad, weight)))


def store_kernel(act, g, act_out, g_out, sems):
    copies = [pltpu.make_async_copy(act, act_out, sems.at[8])]
    for k in range(8):
        rows = pl.ds(k * 96, 96)
        copies.append(pltpu.make_async_copy(g.at[rows], g_out.at[rows], sems.at[k]))
    for copy in copies:
        copy.start()
    for copy in copies:
        copy.wait()


def store(act, g):
    return pl.pallas_call(
        store_kernel,
        out_shape=(jax.ShapeDtypeStruct(act.shape, act.dtype), jax.ShapeDtypeStruct(g.shape, g.dtype)),
        in_specs=[pl.BlockSpec(memory_space=pltpu.VMEM)] * 2,
        out_specs=[pl.BlockSpec(memory_space=pl.ANY)] * 2,
        scratch_shapes=[pltpu.SemaphoreType.DMA((9,))],
        compiler_params=pltpu.CompilerParams(vmem_limit_bytes=12 * 1024 * 1024),
    )(act, g)


def shards(tokens, prev_tokens, hidden_grad, active_blocks, weight):
    act, grad = exchange(active_blocks, tokens, prev_tokens, hidden_grad, weight)
    return tuple(store(act, grad))


def solution(mesh):
    return jax.shard_map(
        shards,
        mesh=mesh,
        in_specs=(P("row", "col"), P("row", "col"), P("col", "row"), P(), P("col", "row")),
        out_specs=(P("col", "row"), P("col", "row")),
        check_vma=False,
    )
```
